32 devices in a mesh: batch: 2 (over x), cols: 4 (over z), rows: 4 (over y, core).
Axes of the slice: x: 2, y: 2, z: 4, core: 2. Of those that a mesh axis runs over, the one named last changes fastest.
Arguments:
- frames: bfloat16 [8, 2, 96, 192, 16], P(None, 'batch', 'rows', 'cols'), parts along dimension 1
- h_init: float32 [2, 96, 192, 256], P('batch', 'rows', 'cols'), parts along dimension 0
- w_x: bfloat16 [3, 3, 16, 768], replicated
- w_hzr: bfloat16 [3, 3, 256, 512], replicated
- w_hn: bfloat16 [3, 3, 256, 256], replicated
- gate_bias: float32 [768], replicated
Outputs:
- output 1: bfloat16 [8, 2, 96, 192, 256], P(None, 'batch', 'rows', 'cols'), parts along dimension 1
- output 2: float32 [2, 96, 192, 256], P('batch', 'rows', 'cols'), parts along dimension 0
There are 2 independent parts. The reference program is written for one: setup_inputs(seed, part) draws one part's arguments, and reference() takes and returns one part's arrays. A program takes and returns all parts, laid end to end along the dimension named above; an argument that names none is the same for every part.
All inputs are finite; a program needn't handle non-finite values.
Results may differ from the reference program's by a relative error of at most 0.00325416.
Values are sent between devices in bfloat16 or wider.
A program may use at most 1 GiB of HBM per device.

```python
import jax
import jax.numpy as jnp
from jax import lax

STEPS = 8
BATCH = 1
HEIGHT = 96
WIDTH = 192
CIN = 16
CH = 256


def setup_inputs(seed: int = 0, part: int = 0) -> dict:
    keys = jax.random.split(jax.random.key(seed), 6)
    key_frames = jax.random.fold_in(keys[0], part)
    key_state = jax.random.fold_in(keys[1], part)
    frames = jax.random.normal(key_frames, (STEPS, BATCH, HEIGHT, WIDTH, CIN), jnp.float32).astype(jnp.bfloat16)
    h_init = 0.8 * jax.random.normal(key_state, (BATCH, HEIGHT, WIDTH, CH), jnp.float32)
    w_x = (jax.random.normal(keys[2], (3, 3, CIN, 3 * CH), jnp.float32) * (9 * CIN) ** -0.5).astype(jnp.bfloat16)
    w_hzr = (jax.random.normal(keys[3], (3, 3, CH, 2 * CH), jnp.float32) * (1.5 * (9 * CH) ** -0.5)).astype(jnp.bfloat16)
    w_hn = (jax.random.normal(keys[4], (3, 3, CH, CH), jnp.float32) * (2.0 * (9 * CH) ** -0.5)).astype(jnp.bfloat16)
    gate_bias = 0.5 * jax.random.normal(keys[5], (3 * CH,), jnp.float32)
    return {'frames': frames, 'h_init': h_init, 'w_x': w_x, 'w_hzr': w_hzr, 'w_hn': w_hn, 'gate_bias': gate_bias}


def conv_same(inputs, weights):
    return lax.conv_general_dilated(inputs.astype(jnp.float32), weights.astype(jnp.float32), (1, 1), 'SAME', dimension_numbers=('NHWC', 'HWIO', 'NHWC'), precision=lax.Precision.HIGHEST)


def reference(frames, h_init, w_x, w_hzr, w_hn, gate_bias):
    def one_step(h_prev, frame_t):
        gate_x = conv_same(frame_t, w_x) + gate_bias
        zr_gates = jax.nn.sigmoid(gate_x[..., :2 * CH] + conv_same(h_prev.astype(jnp.bfloat16), w_hzr))
        update = zr_gates[..., :CH]
        reset_hid = (zr_gates[..., CH:] * h_prev).astype(jnp.bfloat16)
        candidate = jnp.tanh(gate_x[..., 2 * CH:] + conv_same(reset_hid, w_hn))
        h_next = (1.0 - update) * candidate + update * h_prev
        return h_next, h_next.astype(jnp.bfloat16)
    h_last, h_seq = lax.scan(one_step, h_init, frames)
    return h_seq, h_last
```

```python
import jax
import jax.numpy as jnp
from jax import lax
from jax.experimental import pallas as pl
from jax.experimental.pallas import tpu as pltpu
from jax.sharding import PartitionSpec as P

BF16 = jnp.bfloat16
F32 = jnp.float32
MESH = pl.DeviceIdType.MESH
LANES = 128
COL_HALO = 16
CHUNKS = (6, 6, 6, 6)
NAMES = ("batch", "cols", "rows")


def sigmoid(v):
    return 0.5 * jnp.tanh(0.5 * v) + 0.5


def kernel_body(n_cols, n_rows, dims, frames, h_init, w_x, w_hzr, w_hn, bias, h_seq, h_last,
                wzr, wn, wx, bv, fv, fp, hb, rb, xp, xe, af, h32, zb, hf, hl, cs, cr, kr, cb,
                load_sem, fsend, frecv, csend, crecv, ksend, krecv, vsend, vrecv, osem, lsem):
    steps, tile_h, tile_w, cin, ch = dims
    batch = lax.axis_index("batch")
    col = lax.axis_index("cols")
    row = lax.axis_index("rows")
    flip = lax.rem(row, 2)
    first_row = row - 1 + 2 * flip
    last_row = row + 1 - 2 * flip
    has_first = jnp.logical_and(first_row >= 0, first_row < n_rows)
    has_last = jnp.logical_and(last_row >= 0, last_row < n_rows)
    has_left = col > 0
    has_right = col < n_cols - 1
    both = jnp.logical_and
    left_dev = (batch, col - 1, row)
    right_dev = (batch, col + 1, row)
    first_dev = (batch, col, first_row)
    last_dev = (batch, col, last_row)
    corner_ok = (both(has_first, has_left), both(has_first, has_right), both(has_last, has_left), both(has_last, has_right))
    corner_dev = ((batch, col - 1, first_row), (batch, col + 1, first_row), (batch, col - 1, last_row), (batch, col + 1, last_row))
    around = ((has_left, left_dev), (has_right, right_dev), (has_first, first_dev), (has_last, last_dev)) + tuple(zip(corner_ok, corner_dev))

    def phys(i):
        return i + flip * (tile_h - 1 - 2 * i)

    n_chunks = len(CHUNKS)
    starts = [sum(CHUNKS[:k]) for k in range(n_chunks)]
    n_ranges = [(starts[k], CHUNKS[k]) for k in range(n_chunks)]
    r_ranges = []
    for k in range(n_chunks):
        lo = -1 if k == 0 else starts[k] + 1
        hi = tile_h + 1 if k == n_chunks - 1 else starts[k] + CHUNKS[k] + 1
        r_ranges.append((lo, hi - lo))

    def remote(src, dst, s_sem, r_sem, dev):
        return pltpu.make_async_remote_copy(src_ref=src, dst_ref=dst, send_sem=s_sem, recv_sem=r_sem, device_id=dev, device_id_type=MESH)

    loads = []
    for i in range(tile_h):
        loads.append(pltpu.make_async_copy(h_init.at[0, phys(i)], h32.at[i], load_sem.at[0, i]))
    frame_loads = [pltpu.make_async_copy(frames.at[:, 0, phys(i)], fv.at[i], load_sem.at[1, i]) for i in range(tile_h)]
    weight_loads = []
    for a in range(3):
        la = a + flip * (2 - 2 * a)
        weight_loads.append(pltpu.make_async_copy(w_hzr.at[a], wzr.at[la], load_sem.at[2, a]))
        weight_loads.append(pltpu.make_async_copy(w_hn.at[a], wn.at[la], load_sem.at[2, 3 + a]))
        for c in range(3):
            dst = wx.at[pl.ds(pl.multiple_of(64 * c + cin * la, cin), cin)]
            weight_loads.append(pltpu.make_async_copy(w_x.at[a, c], dst, load_sem.at[2, 6 + 3 * a + c]))
    weight_loads.append(pltpu.make_async_copy(bias, bv, load_sem.at[2, 15]))
    for copy in frame_loads + loads + weight_loads:
        copy.start()

    hf[...] = jnp.zeros_like(hf)
    hl[...] = jnp.zeros_like(hl)
    cr[...] = jnp.zeros_like(cr)
    kr[...] = jnp.zeros_like(kr)
    cb[...] = jnp.zeros_like(cb)
    cs[...] = jnp.zeros_like(cs)
    fp[...] = jnp.zeros_like(fp)
    for lo, hi in ((48, 64), (112, 128), (176, 256)):
        wx[lo:hi] = jnp.zeros((hi - lo, 3 * ch), BF16)

    barrier = pltpu.get_barrier_semaphore()
    count = 0
    for ok, dev in around:
        count = count + ok.astype(jnp.int32)

        @pl.when(ok)
        def _(dev=dev):
            pl.semaphore_signal(barrier, inc=1, device_id=dev, device_id_type=MESH)
    pl.semaphore_wait(barrier, count)

    lane = lax.broadcasted_iota(jnp.int32, (1, LANES), 1)

    for copy in frame_loads:
        copy.wait()
    own_c = pl.ds(COL_HALO, tile_w)
    for i in range(tile_h):
        fp[i + 2, own_c] = fv[i].reshape(steps * cin, tile_w).astype(F32).T.astype(BF16)

    lo_c = pl.ds(0, COL_HALO)
    hi_c = pl.ds(COL_HALO + tile_w, COL_HALO)
    own_lo = pl.ds(COL_HALO, COL_HALO)
    own_hi = pl.ds(tile_w, COL_HALO)
    f_copies = []
    own_r = pl.ds(2, tile_h)
    f_copies.append((has_left, fp.at[own_r, own_lo], fp.at[own_r, hi_c], left_dev))
    f_copies.append((has_right, fp.at[own_r, own_hi], fp.at[own_r, lo_c], right_dev))
    for ok, okl, okr, dev, cdl, cdr, rows in (
            (has_first, corner_ok[0], corner_ok[1], first_dev, corner_dev[0], corner_dev[1], ((2, 1), (3, 0))),
            (has_last, corner_ok[2], corner_ok[3], last_dev, corner_dev[2], corner_dev[3], ((tile_h + 1, tile_h + 2), (tile_h, tile_h + 3)))):
        for src, dst in rows:
            f_copies.append((ok, fp.at[src, own_c], fp.at[dst, own_c], dev))
            f_copies.append((okl, fp.at[src, own_lo], fp.at[dst, hi_c], cdl))
            f_copies.append((okr, fp.at[src, own_hi], fp.at[dst, lo_c], cdr))
    f_recv_index = [1, 0]
    for g in range(4):
        f_recv_index += [2 + 3 * g, 4 + 3 * g, 3 + 3 * g]
    f_descs = [(ok, remote(s, d, fsend.at[m], frecv.at[f_recv_index[m]], dev)) for m, (ok, s, d, dev) in enumerate(f_copies)]
    for ok, copy in f_descs:
        @pl.when(ok)
        def _(copy=copy):
            copy.start()

    def col_sends(k, slot):
        out = [(has_left, remote(cs.at[k, pl.ds(0, 2)], cr.at[slot, 1, k], csend.at[0, k], crecv.at[slot, 1, k], left_dev)),
               (has_right, remote(cs.at[k, pl.ds(2, 2)], cr.at[slot, 0, k], csend.at[1, k], crecv.at[slot, 0, k], right_dev))]
        if k == 0:
            out.append((has_first, remote(h32.at[pl.ds(0, 2)], hf.at[slot], vsend.at[0], vrecv.at[slot, 0], first_dev)))
            out.append((corner_ok[0], remote(cs.at[k, pl.ds(0, 2)], kr.at[slot, 1], ksend.at[0], krecv.at[slot, 1], corner_dev[0])))
            out.append((corner_ok[1], remote(cs.at[k, pl.ds(2, 2)], kr.at[slot, 0], ksend.at[1], krecv.at[slot, 0], corner_dev[1])))
        if k == n_chunks - 1:
            out.append((has_last, remote(h32.at[pl.ds(tile_h - 2, 2)], hl.at[slot], vsend.at[1], vrecv.at[slot, 1], last_dev)))
            out.append((corner_ok[2], remote(cs.at[k, pl.ds(0, 2)], kr.at[slot, 3], ksend.at[2], krecv.at[slot, 3], corner_dev[2])))
            out.append((corner_ok[3], remote(cs.at[k, pl.ds(2, 2)], kr.at[slot, 2], ksend.at[3], krecv.at[slot, 2], corner_dev[3])))
        return out

    def start_sends(k, slot, more):
        for ok, copy in col_sends(k, slot):
            @pl.when(both(ok, more))
            def _(copy=copy):
                copy.start()

    def wait_sends(k, slot):
        for ok, copy in col_sends(k, slot):
            @pl.when(ok)
            def _(copy=copy):
                copy.wait_send()

    def wait_if(ok, dst, sem, src):
        @pl.when(ok)
        def _():
            remote(src, dst, csend.at[0, 0], sem, right_dev).wait_recv()

    sub48 = lax.broadcasted_iota(jnp.int32, (tile_w, ch), 0)
    sub16 = lax.broadcasted_iota(jnp.int32, (16, ch), 0)

    def row_of(colbuf, i):
        return cb[colbuf, pl.ds(i + 8, 1), :]

    def publish(slot, i, v, k):
        hb[slot, 1, i + 2] = v.astype(BF16)
        hb[slot, 0, i + 2] = pltpu.roll(v, 1, 0).astype(BF16)
        hb[slot, 2, i + 2] = pltpu.roll(v, tile_w - 1, 0).astype(BF16)
        j = i - starts[k]
        for q, x in enumerate((0, 1, tile_w - 2, tile_w - 1)):
            cs[k, q, pl.ds(j, 1), :] = v[x:x + 1]
        cb[2, pl.ds(i + 8, 1), :] = v[0:1]
        cb[3, pl.ds(i + 8, 1), :] = v[tile_w - 1:tile_w]

    def arrive_cols(slot, k):
        wait_if(has_left, cr.at[slot, 0, k], crecv.at[slot, 0, k], cs.at[k, pl.ds(0, 2)])
        wait_if(has_right, cr.at[slot, 1, k], crecv.at[slot, 1, k], cs.at[k, pl.ds(0, 2)])
        i0, n = n_ranges[k]
        for side in range(2):
            for m in range(2):
                cb[4 * side + m, pl.ds(i0 + 8, n), :] = cr[slot, side, k, m, 0:n, :]
        for i in range(i0, i0 + n):
            old = hb[slot, 0, i + 2, 0:16].astype(F32)
            hb[slot, 0, i + 2, 0:16] = jnp.where(sub16 == 0, row_of(1, i), old).astype(BF16)
            old = hb[slot, 2, i + 2, tile_w - 16:tile_w].astype(F32)
            hb[slot, 2, i + 2, tile_w - 16:tile_w] = jnp.where(sub16 == 15, row_of(4, i), old).astype(BF16)

    def arrive_rows(slot, last):
        src, ok = (hl, has_last) if last else (hf, has_first)
        wait_if(ok, src.at[slot], vrecv.at[slot, last], h32.at[pl.ds(0, 2)])
        for m in range(2):
            q = 2 * last + m
            wait_if(corner_ok[q], kr.at[slot, q], krecv.at[slot, q], cs.at[0, pl.ds(0, 2)])
        for depth in range(2):
            i = tile_h + depth if last else -1 - depth
            m = 1 - depth if last else depth
            j = CHUNKS[-1] - 1 - depth if last else depth
            for x in range(2):
                cb[x, pl.ds(i + 8, 1), :] = kr[slot, 2 * last, x, j:j + 1, :]
                cb[4 + x, pl.ds(i + 8, 1), :] = kr[slot, 2 * last + 1, x, j:j + 1, :]
            v = src[slot, m]
            cb[2, pl.ds(i + 8, 1), :] = v[0:1]
            cb[3, pl.ds(i + 8, 1), :] = v[tile_w - 1:tile_w]
            hb[slot, 1, i + 2] = v.astype(BF16)
            hb[slot, 0, i + 2] = jnp.where(sub48 == 0, row_of(1, i), pltpu.roll(v, 1, 0)).astype(BF16)
            hb[slot, 2, i + 2] = jnp.where(sub48 == tile_w - 1, row_of(4, i), pltpu.roll(v, tile_w - 1, 0)).astype(BF16)

    wide = tile_w + 2 * COL_HALO

    def build_x(t, slot, k):
        i0, n = r_ranges[k]
        for j in range(n):
            parts = [pltpu.roll(fp[i0 + j + a + 1].astype(F32), lax.rem(cin * a - cin * t + cin * steps, cin * steps), 1) for a in range(3)]
            af[pl.ds(j * wide, wide)] = jnp.where(lane < cin, parts[0], jnp.where(lane < 2 * cin, parts[1], parts[2]))
        for j in range(n):
            base = j * wide + COL_HALO
            left = af[pl.ds(base - 1, tile_w)]
            mid = pltpu.roll(af[pl.ds(base, tile_w)], 64, 1)
            xp[slot, i0 + j + 1, :, 0:LANES] = jnp.where(lane < 64, left, mid).astype(BF16)
            xp[slot, i0 + j + 1, :, LANES:2 * LANES] = af[pl.ds(base + 1, tile_w)].astype(BF16)
        lo_half, hi_half = [], []
        for x in (-1, tile_w):
            three = [af[pl.ds(COL_HALO + x + c - 1, 8, wide)] for c in range(3)]
            lo_half.append(jnp.where(lane < 64, three[0], pltpu.roll(three[1], 64, 1)))
            hi_half.append(three[2])
        xe[slot, k, :, 0:LANES] = jnp.concatenate(lo_half, axis=0).astype(BF16)
        xe[slot, k, :, LANES:2 * LANES] = jnp.concatenate(hi_half, axis=0).astype(BF16)

    def conv(src, i0, n, off, weights, xslot, gate, extra=None):
        lo, w_lo = gate * ch, (0 if gate == 2 else gate * ch)
        acc = None
        for c in (1, 0, 2):
            for a in range(3):
                lhs = src(c, pl.ds(i0 + a - 1 - off, n)).reshape(n * tile_w, ch)
                if extra is not None:
                    ends = [cb[3 * side + c, pl.ds(i0 + a - 1 + 8, 8), :] for side in range(2)]
                    lhs = jnp.concatenate([lhs, jnp.concatenate(ends, axis=0).astype(BF16)], axis=0)
                part = jnp.dot(lhs, weights[a, c, :, w_lo:w_lo + ch], preferred_element_type=F32)
                acc = part if acc is None else acc + part
        lhs = xp[xslot, pl.ds(i0 + 1, n)].reshape(n * tile_w, ch)
        if extra is not None:
            lhs = jnp.concatenate([lhs, xe[xslot, extra]], axis=0)
        acc = acc + jnp.dot(lhs, wx[:, lo:lo + ch], preferred_element_type=F32)
        return acc + bv[:, lo:lo + ch]

    for copy in loads:
        copy.wait()
    for k in range(n_chunks):
        i0, n = n_ranges[k]
        for i in range(i0, i0 + n):
            publish(0, i, h32[i], k)
        start_sends(k, 0, True)
    for m, (ok, copy) in enumerate(f_descs):
        src, dst = f_copies[m][1], f_copies[f_recv_index[m]][2]

        @pl.when(ok)
        def _(copy=copy, m=m, src=src, dst=dst):
            copy.wait_send()
            remote(src, dst, fsend.at[m], frecv.at[m], right_dev).wait_recv()
    for k in range(n_chunks):
        build_x(0, 0, k)
    for copy in weight_loads:
        copy.wait()

    def out_copy(t, slot, i):
        return pltpu.make_async_copy(hb.at[slot, 1, i + 2], h_seq.at[t, 0, phys(i)], osem.at[slot, i])

    def step(t, carry):
        now = lax.rem(t, 2)
        new = 1 - now
        more = t < steps - 1
        for k in range(n_chunks):
            if k == 0:
                arrive_cols(now, 0)
                arrive_rows(now, 0)
            if k + 1 < n_chunks:
                arrive_cols(now, k + 1)
            else:
                arrive_rows(now, 1)
            i0, n = r_ranges[k]
            acc = conv(lambda c, rows: hb[now, c, rows], i0, n, -2, wzr, now, 1, extra=k)
            if k > 0:
                start_sends(k - 1, new, more)
            gate = sigmoid(acc)
            ends = gate[n * tile_w:]
            ends_l = ends[0:8] * cb[1, pl.ds(i0 + 8, 8), :]
            ends_r = ends[8:16] * cb[4, pl.ds(i0 + 8, 8), :]
            for j in range(n):
                i = i0 + j
                old = hf[now, 0] if i == -1 else hl[now, 1] if i == tile_h else h32[i]
                v = gate[j * tile_w:(j + 1) * tile_w] * old
                rb[1, i + 1] = v.astype(BF16)
                rb[0, i + 1] = jnp.where(sub48 == 0, ends_l[j:j + 1], pltpu.roll(v, 1, 0)).astype(BF16)
                rb[2, i + 1] = jnp.where(sub48 == tile_w - 1, ends_r[j:j + 1], pltpu.roll(v, tile_w - 1, 0)).astype(BF16)
            i0, n = n_ranges[k]
            zb[pl.ds(0, n * tile_w)] = sigmoid(conv(lambda c, rows: hb[now, c, rows], i0, n, -2, wzr, now, 0))

            build_x(jnp.minimum(t + 1, steps - 1), new, k)
            cand = jnp.tanh(conv(lambda c, rows: rb[c, rows], i0, n, -1, wn, now, 2))
            wait_sends(k, now)
            for i in range(i0, i0 + n):
                @pl.when(t >= 2)
                def _(i=i):
                    out_copy(t, new, i).wait()
            for j in range(n):
                i = i0 + j
                mix = cand[j * tile_w:(j + 1) * tile_w]
                v = mix + zb[pl.ds(j * tile_w, tile_w)] * (h32[i] - mix)
                h32[i] = v
                publish(new, i, v, k)
            for i in range(i0, i0 + n):
                out_copy(t, new, i).start()
        start_sends(n_chunks - 1, new, more)
        return carry

    lax.fori_loop(0, steps, step, 0)
    finals = [pltpu.make_async_copy(h32.at[i], h_last.at[0, phys(i)], lsem.at[i]) for i in range(tile_h)]
    for copy in finals:
        copy.start()
    for slot in range(2):
        for i in range(tile_h):
            out_copy(0, slot, i).wait()
    for copy in finals:
        copy.wait()


def solution(mesh):
    n_rows, n_cols = mesh.shape["rows"], mesh.shape["cols"]
    frame_spec = P(None, "batch", "rows", "cols", None)
    state_spec = P("batch", "rows", "cols", None)

    def local_fn(frames, h_init, w_x, w_hzr, w_hn, gate_bias):
        steps, _, tile_h, tile_w, cin = frames.shape
        ch = h_init.shape[-1]
        dims = (steps, tile_h, tile_w, cin, ch)
        vm = pltpu.VMEM
        dma = pltpu.SemaphoreType.DMA
        kk = len(CHUNKS)
        wide = tile_w + 2 * COL_HALO
        scratch = [
            vm((3, 3, ch, 2 * ch), BF16), vm((3, 3, ch, ch), BF16), vm((256, 3 * ch), BF16), vm((1, 3 * ch), F32),
            vm((tile_h, steps, cin, tile_w), BF16), vm((tile_h + 4, wide, LANES), BF16),
            vm((2, 3, tile_h + 4, tile_w, ch), BF16), vm((3, tile_h + 2, tile_w, ch), BF16),
            vm((2, tile_h + 2, tile_w, ch), BF16), vm((2, kk, 16, ch), BF16), vm((8 * wide, LANES), F32),
            vm((tile_h, tile_w, ch), F32), vm((max(CHUNKS) * tile_w, ch), F32),
            vm((2, 2, tile_w, ch), F32), vm((2, 2, tile_w, ch), F32),
            vm((kk, 4, 8, ch), F32), vm((2, 2, kk, 2, 8, ch), F32), vm((2, 4, 2, 8, ch), F32), vm((6, 48, ch), F32),
            dma((3, tile_h)), dma((14,)), dma((14,)), dma((2, kk)), dma((2, 2, kk)), dma((4,)), dma((2, 4)),
            dma((2,)), dma((2, 2)), dma((2, tile_h)), dma((tile_h,)),
        ]

        def body(*refs):
            kernel_body(n_cols, n_rows, dims, *refs)

        return pl.pallas_call(
            body,
            out_shape=(jax.ShapeDtypeStruct((steps, 1, tile_h, tile_w, ch), BF16), jax.ShapeDtypeStruct((1, tile_h, tile_w, ch), F32)),
            in_specs=[pl.BlockSpec(memory_space=pl.ANY)] * 6,
            out_specs=(pl.BlockSpec(memory_space=pl.ANY),) * 2,
            scratch_shapes=scratch,
            compiler_params=pltpu.CompilerParams(collective_id=0, has_side_effects=True, vmem_limit_bytes=56 * 1024 * 1024),
            name="convgru",
        )(jnp.swapaxes(frames, 3, 4), h_init, w_x, w_hzr, w_hn, gate_bias.reshape(1, -1))

    return jax.shard_map(local_fn, mesh=mesh, in_specs=(frame_spec, state_spec, P(), P(), P(), P()), out_specs=(frame_spec, state_spec), check_vma=False)
```

```python
import jax
import jax.numpy as jnp
from jax import lax
from jax.experimental import pallas as pl
from jax.experimental.pallas import tpu as pltpu
from jax.sharding import PartitionSpec as P

BF16 = jnp.bfloat16
F32 = jnp.float32
MESH = pl.DeviceIdType.MESH
LANES = 128
COL_HALO = 16
CHUNKS = (6,) * 4
UNROLL = 2
NAMES = ("batch", "cols", "rows")


def sigmoid(v):
    return 0.5 * jnp.tanh(0.5 * v) + 0.5


def kernel_body(n_cols, n_rows, dims, frames, h_init, w_x, w_hzr, w_hn, bias, h_seq, h_last,
                wzr, wn, wx, bv, fv, fp, hb, rb, xp, xe, af, h32, zb, hf, hl, cs, cr, kr, cb,
                load_sem, fsend, frecv, csend, crecv, ksend, krecv, vsend, vrecv, osem, lsem):
    steps, tile_h, tile_w, cin, ch = dims
    batch = lax.axis_index("batch")
    col = lax.axis_index("cols")
    row = lax.axis_index("rows")
    flip = lax.rem(row, 2)
    first_row = row - 1 + 2 * flip
    last_row = row + 1 - 2 * flip
    has_first = jnp.logical_and(first_row >= 0, first_row < n_rows)
    has_last = jnp.logical_and(last_row >= 0, last_row < n_rows)
    has_left = col > 0
    has_right = col < n_cols - 1
    both = jnp.logical_and
    left_dev = (batch, col - 1, row)
    right_dev = (batch, col + 1, row)
    first_dev = (batch, col, first_row)
    last_dev = (batch, col, last_row)
    corner_ok = (both(has_first, has_left), both(has_first, has_right), both(has_last, has_left), both(has_last, has_right))
    corner_dev = ((batch, col - 1, first_row), (batch, col + 1, first_row), (batch, col - 1, last_row), (batch, col + 1, last_row))
    around = ((has_left, left_dev), (has_right, right_dev), (has_first, first_dev), (has_last, last_dev)) + tuple(zip(corner_ok, corner_dev))

    def phys(i):
        return i + flip * (tile_h - 1 - 2 * i)

    n_chunks = len(CHUNKS)
    starts = [sum(CHUNKS[:k]) for k in range(n_chunks)]
    n_ranges = [(starts[k], CHUNKS[k]) for k in range(n_chunks)]
    r_ranges = []
    for k in range(n_chunks):
        lo = -1 if k == 0 else starts[k] + 1
        hi = tile_h + 1 if k == n_chunks - 1 else starts[k] + CHUNKS[k] + 1
        r_ranges.append((lo, hi - lo))

    def remote(src, dst, s_sem, r_sem, dev):
        return pltpu.make_async_remote_copy(src_ref=src, dst_ref=dst, send_sem=s_sem, recv_sem=r_sem, device_id=dev, device_id_type=MESH)

    loads = []
    for i in range(tile_h):
        loads.append(pltpu.make_async_copy(h_init.at[0, phys(i)], h32.at[i], load_sem.at[0, i]))
    frame_loads = [pltpu.make_async_copy(frames.at[:, 0, phys(i)], fv.at[i], load_sem.at[1, i]) for i in range(tile_h)]
    weight_loads = []
    for a in range(3):
        la = a + flip * (2 - 2 * a)
        weight_loads.append(pltpu.make_async_copy(w_hzr.at[a], wzr.at[la], load_sem.at[2, a]))
        weight_loads.append(pltpu.make_async_copy(w_hn.at[a], wn.at[la], load_sem.at[2, 3 + a]))
        for c in range(3):
            dst = wx.at[pl.ds(pl.multiple_of(64 * c + cin * la, cin), cin)]
            weight_loads.append(pltpu.make_async_copy(w_x.at[a, c], dst, load_sem.at[2, 6 + 3 * a + c]))
    weight_loads.append(pltpu.make_async_copy(bias, bv, load_sem.at[2, 15]))
    for copy in frame_loads + loads + weight_loads:
        copy.start()

    hf[...] = jnp.zeros_like(hf)
    hl[...] = jnp.zeros_like(hl)
    cr[...] = jnp.zeros_like(cr)
    kr[...] = jnp.zeros_like(kr)
    cb[...] = jnp.zeros_like(cb)
    cs[...] = jnp.zeros_like(cs)
    fp[...] = jnp.zeros_like(fp)
    for lo, hi in ((48, 64), (112, 128), (176, 256)):
        wx[lo:hi] = jnp.zeros((hi - lo, 3 * ch), BF16)

    barrier = pltpu.get_barrier_semaphore()
    count = 0
    for ok, dev in around:
        count = count + ok.astype(jnp.int32)

        @pl.when(ok)
        def _(dev=dev):
            pl.semaphore_signal(barrier, inc=1, device_id=dev, device_id_type=MESH)
    pl.semaphore_wait(barrier, count)

    lane = lax.broadcasted_iota(jnp.int32, (1, LANES), 1)

    for copy in frame_loads:
        copy.wait()
    own_c = pl.ds(COL_HALO, tile_w)
    for i in range(tile_h):
        fp[i + 2, own_c] = fv[i].reshape(steps * cin, tile_w).astype(F32).T.astype(BF16)

    lo_c = pl.ds(0, COL_HALO)
    hi_c = pl.ds(COL_HALO + tile_w, COL_HALO)
    own_lo = pl.ds(COL_HALO, COL_HALO)
    own_hi = pl.ds(tile_w, COL_HALO)
    f_copies = []
    own_r = pl.ds(2, tile_h)
    f_copies.append((has_left, fp.at[own_r, own_lo], fp.at[own_r, hi_c], left_dev))
    f_copies.append((has_right, fp.at[own_r, own_hi], fp.at[own_r, lo_c], right_dev))
    for ok, okl, okr, dev, cdl, cdr, rows in (
            (has_first, corner_ok[0], corner_ok[1], first_dev, corner_dev[0], corner_dev[1], ((2, 1), (3, 0))),
            (has_last, corner_ok[2], corner_ok[3], last_dev, corner_dev[2], corner_dev[3], ((tile_h + 1, tile_h + 2), (tile_h, tile_h + 3)))):
        for src, dst in rows:
            f_copies.append((ok, fp.at[src, own_c], fp.at[dst, own_c], dev))
            f_copies.append((okl, fp.at[src, own_lo], fp.at[dst, hi_c], cdl))
            f_copies.append((okr, fp.at[src, own_hi], fp.at[dst, lo_c], cdr))
    f_recv_index = [1, 0]
    for g in range(4):
        f_recv_index += [2 + 3 * g, 4 + 3 * g, 3 + 3 * g]
    f_descs = [(ok, remote(s, d, fsend.at[m], frecv.at[f_recv_index[m]], dev)) for m, (ok, s, d, dev) in enumerate(f_copies)]
    for ok, copy in f_descs:
        @pl.when(ok)
        def _(copy=copy):
            copy.start()

    def chunk_sends(k, slot):
        to_left = cs.at[slot, k, 0]
        to_right = cs.at[slot, k, 1]
        out = [(has_left, remote(to_left, cr.at[slot, 1, k], csend.at[slot, 0, k], crecv.at[slot, 1, k], left_dev)),
               (has_right, remote(to_right, cr.at[slot, 0, k], csend.at[slot, 1, k], crecv.at[slot, 0, k], right_dev))]
        for edge, q in ((0, 0), (n_chunks - 1, 2)):
            if k == edge:
                out.append((corner_ok[q], remote(to_left, kr.at[slot, q + 1], ksend.at[slot, q], krecv.at[slot, q + 1], corner_dev[q])))
                out.append((corner_ok[q + 1], remote(to_right, kr.at[slot, q], ksend.at[slot, q + 1], krecv.at[slot, q], corner_dev[q + 1])))
        return out

    def row_send(k, slot):
        if k == 0:
            return has_first, remote(h32.at[pl.ds(0, 2)], hf.at[slot], vsend.at[0], vrecv.at[slot, 0], first_dev)
        return has_last, remote(h32.at[pl.ds(tile_h - 2, 2)], hl.at[slot], vsend.at[1], vrecv.at[slot, 1], last_dev)

    def start_sends(k, slot, more):
        copies = chunk_sends(k, slot)
        if k in (0, n_chunks - 1):
            copies.append(row_send(k, slot))
        for ok, copy in copies:
            @pl.when(both(ok, more))
            def _(copy=copy):
                copy.start()

    def wait_chunk_sends(slot, cond):
        for k in range(n_chunks):
            for ok, copy in chunk_sends(k, slot):
                @pl.when(both(ok, cond))
                def _(copy=copy):
                    copy.wait_send()

    def wait_row_send(k, slot):
        ok, copy = row_send(k, slot)

        @pl.when(ok)
        def _():
            copy.wait_send()

    def wait_if(ok, dst, sem, src):
        @pl.when(ok)
        def _():
            remote(src, dst, csend.at[0, 0, 0], sem, right_dev).wait_recv()

    sub48 = lax.broadcasted_iota(jnp.int32, (tile_w, ch), 0)
    sub16 = lax.broadcasted_iota(jnp.int32, (16, ch), 0)

    def row_of(colbuf, i):
        return cb[colbuf, pl.ds(i + 8, 1), :]

    def publish(slot, i, v, k):
        hb[slot, 1, i + 2] = v.astype(BF16)
        hb[slot, 0, i + 2] = pltpu.roll(v, 1, 0).astype(BF16)
        hb[slot, 2, i + 2] = pltpu.roll(v, tile_w - 1, 0).astype(BF16)
        j = i - starts[k]
        for side, m, x in ((0, 0, 0), (0, 1, 1), (1, 0, tile_w - 2), (1, 1, tile_w - 1)):
            cs[slot, k, side, pl.ds(8 * m + j, 1), :] = v[x:x + 1]
        cb[2, pl.ds(i + 8, 1), :] = v[0:1]
        cb[3, pl.ds(i + 8, 1), :] = v[tile_w - 1:tile_w]

    def wait_cols(slot, k):
        wait_if(has_left, cr.at[slot, 0, k], crecv.at[slot, 0, k], cs.at[slot, k, 0])
        wait_if(has_right, cr.at[slot, 1, k], crecv.at[slot, 1, k], cs.at[slot, k, 0])

    def place_cols(slot, k):
        i0, n = n_ranges[k]
        for side in range(2):
            for m in range(2):
                cb[4 * side + m, pl.ds(i0 + 8, n), :] = cr[slot, side, k, 8 * m:8 * m + n, :]
        for i in range(i0, i0 + n):
            old = hb[slot, 0, i + 2, 0:16].astype(F32)
            hb[slot, 0, i + 2, 0:16] = jnp.where(sub16 == 0, row_of(1, i), old).astype(BF16)
            old = hb[slot, 2, i + 2, tile_w - 16:tile_w].astype(F32)
            hb[slot, 2, i + 2, tile_w - 16:tile_w] = jnp.where(sub16 == 15, row_of(4, i), old).astype(BF16)

    def wait_rows(slot, last):
        src, ok = (hl, has_last) if last else (hf, has_first)
        wait_if(ok, src.at[slot], vrecv.at[slot, last], h32.at[pl.ds(0, 2)])
        for m in range(2):
            q = 2 * last + m
            wait_if(corner_ok[q], kr.at[slot, q], krecv.at[slot, q], cs.at[slot, 0, 0])

    def place_rows(slot, last):
        src = hl if last else hf
        for depth in range(2):
            i = tile_h + depth if last else -1 - depth
            m = 1 - depth if last else depth
            j = CHUNKS[-1] - 1 - depth if last else depth
            for x in range(2):
                cb[x, pl.ds(i + 8, 1), :] = kr[slot, 2 * last, 8 * x + j:8 * x + j + 1, :]
                cb[4 + x, pl.ds(i + 8, 1), :] = kr[slot, 2 * last + 1, 8 * x + j:8 * x + j + 1, :]
            v = src[slot, m]
            cb[2, pl.ds(i + 8, 1), :] = v[0:1]
            cb[3, pl.ds(i + 8, 1), :] = v[tile_w - 1:tile_w]
            hb[slot, 1, i + 2] = v.astype(BF16)
            hb[slot, 0, i + 2] = jnp.where(sub48 == 0, row_of(1, i), pltpu.roll(v, 1, 0)).astype(BF16)
            hb[slot, 2, i + 2] = jnp.where(sub48 == tile_w - 1, row_of(4, i), pltpu.roll(v, tile_w - 1, 0)).astype(BF16)

    wide = tile_w + 2 * COL_HALO

    def build_x(t, slot, k):
        i0, n = r_ranges[k]
        for j in range(n):
            parts = [pltpu.roll(fp[i0 + j + a + 1].astype(F32), lax.rem(cin * a - cin * t + cin * steps, cin * steps), 1) for a in range(3)]
            af[pl.ds(j * wide, wide)] = jnp.where(lane < cin, parts[0], jnp.where(lane < 2 * cin, parts[1], parts[2]))
        for j in range(n):
            base = j * wide + COL_HALO
            left = af[pl.ds(base - 1, tile_w)]
            mid = pltpu.roll(af[pl.ds(base, tile_w)], 64, 1)
            xp[slot, i0 + j + 1, :, 0:LANES] = jnp.where(lane < 64, left, mid).astype(BF16)
            xp[slot, i0 + j + 1, :, LANES:2 * LANES] = af[pl.ds(base + 1, tile_w)].astype(BF16)
        lo_half, hi_half = [], []
        for x in (-1, tile_w):
            three = [af[pl.ds(COL_HALO + x + c - 1, 8, wide)] for c in range(3)]
            lo_half.append(jnp.where(lane < 64, three[0], pltpu.roll(three[1], 64, 1)))
            hi_half.append(three[2])
        xe[slot, k, :, 0:LANES] = jnp.concatenate(lo_half, axis=0).astype(BF16)
        xe[slot, k, :, LANES:2 * LANES] = jnp.concatenate(hi_half, axis=0).astype(BF16)

    def conv(src, i0, n, off, weights, xslot, gate, extra=None, e_lo=0):
        lo, w_lo = gate * ch, (0 if gate == 2 else gate * ch)
        acc = None
        for c in (1, 0, 2):
            for a in range(3):
                lhs = src(c, pl.ds(i0 + a - 1 - off, n)).reshape(n * tile_w, ch)
                if extra is not None:
                    ends = [cb[3 * side + c, pl.ds(e_lo + a - 1 + 8, 8), :] for side in range(2)]
                    lhs = jnp.concatenate([lhs, jnp.concatenate(ends, axis=0).astype(BF16)], axis=0)
                part = jnp.dot(lhs, weights[a, c, :, w_lo:w_lo + ch], preferred_element_type=F32)
                acc = part if acc is None else acc + part
        lhs = xp[xslot, pl.ds(i0 + 1, n)].reshape(n * tile_w, ch)
        if extra is not None:
            lhs = jnp.concatenate([lhs, xe[xslot, extra]], axis=0)
        acc = acc + jnp.dot(lhs, wx[:, lo:lo + ch], preferred_element_type=F32)
        return acc + bv[lo:lo + ch].reshape(1, ch)

    for copy in loads:
        copy.wait()
    for k in range(n_chunks):
        i0, n = n_ranges[k]
        for i in range(i0, i0 + n):
            publish(0, i, h32[i], k)
        start_sends(k, 0, True)
    for m, (ok, copy) in enumerate(f_descs):
        src, dst = f_copies[m][1], f_copies[f_recv_index[m]][2]

        @pl.when(ok)
        def _(copy=copy, m=m, src=src, dst=dst):
            copy.wait_send()
            remote(src, dst, fsend.at[m], frecv.at[m], right_dev).wait_recv()
    for k in range(n_chunks):
        build_x(0, 0, k)
    for copy in weight_loads:
        copy.wait()

    def out_copy(t, slot, i):
        return pltpu.make_async_copy(hb.at[slot, 1, i + 2], h_seq.at[t, 0, phys(i)], osem.at[slot, i])

    def halves(i0, n):
        return (i0, n - n // 2), (i0 + n - n // 2, n // 2)

    def meet(t, now, k):
        new = 1 - now
        if k == 0:
            start_sends(n_chunks - 1, now, both(t > 0, True))
            last_outs(t - 1, now, n_chunks - 1, t > 0)
            free_slot(t, now)
            wait_cols(now, 0)
            wait_rows(now, 0)
            wait_row_send(0, now)
        else:
            start_sends(k - 1, new, t < steps - 1)
            last_outs(t, new, k - 1, True)
        if k + 1 < n_chunks:
            wait_cols(now, k + 1)
        else:
            wait_rows(now, 1)
            wait_row_send(n_chunks - 1, now)
        if k == 0:
            place_cols(now, 0)
            place_rows(now, 0)
        if k + 1 < n_chunks:
            place_cols(now, k + 1)
        else:
            place_rows(now, 1)

    def last_outs(t, slot, k, cond):
        for i in range(n_ranges[k][0], sum(n_ranges[k])):
            @pl.when(cond)
            def _(i=i):
                out_copy(t, slot, i).start()

    def free_slot(t, now):
        new = 1 - now
        wait_chunk_sends(new, t >= 1)
        for i in range(tile_h):
            @pl.when(t >= 2)
            def _(i=i):
                out_copy(t, new, i).wait()

    def stretch(t, now, k):
        new = 1 - now
        meet(t, now, k)
        r_lo, r_n = r_ranges[k]
        parts = halves(r_lo, r_n)
        accs = [conv(lambda c, rows: hb[now, c, rows], i0, n, -2, wzr, now, 1, extra=k if h == 1 else None, e_lo=r_lo) for h, (i0, n) in enumerate(parts)]
        gates = [sigmoid(acc) for acc in accs]
        ends = gates[1][parts[1][1] * tile_w:]
        ends_l = ends[0:8] * cb[1, pl.ds(r_lo + 8, 8), :]
        ends_r = ends[8:16] * cb[4, pl.ds(r_lo + 8, 8), :]
        for (i0, n), gate in zip(parts, gates):
            for j in range(n):
                i = i0 + j
                e = i - r_lo
                old = hf[now, 0] if i == -1 else hl[now, 1] if i == tile_h else h32[i]
                v = gate[j * tile_w:(j + 1) * tile_w] * old
                rb[1, i + 1] = v.astype(BF16)
                rb[0, i + 1] = jnp.where(sub48 == 0, ends_l[e:e + 1], pltpu.roll(v, 1, 0)).astype(BF16)
                rb[2, i + 1] = jnp.where(sub48 == tile_w - 1, ends_r[e:e + 1], pltpu.roll(v, tile_w - 1, 0)).astype(BF16)
        parts = halves(*n_ranges[k])
        accs = [conv(lambda c, rows: hb[now, c, rows], i0, n, -2, wzr, now, 0) for i0, n in parts]
        for (i0, n), acc in zip(parts, accs):
            zb[pl.ds((i0 - n_ranges[k][0]) * tile_w, n * tile_w)] = sigmoid(acc)
        build_x(jnp.minimum(t + 1, steps - 1), new, k)
        accs = [conv(lambda c, rows: rb[c, rows], i0, n, -1, wn, now, 2) for i0, n in parts]
        for (i0, n), acc in zip(parts, accs):
            cand = jnp.tanh(acc)
            for j in range(n):
                i = i0 + j
                mix = cand[j * tile_w:(j + 1) * tile_w]
                v = mix + zb[pl.ds((i - n_ranges[k][0]) * tile_w, tile_w)] * (h32[i] - mix)
                h32[i] = v
                publish(new, i, v, k)

    def body(p, carry):
        for s in range(UNROLL):
            for k in range(n_chunks):
                stretch(UNROLL * p + s, s % 2, k)
        return carry

    lax.fori_loop(0, steps // UNROLL, body, 0)
    wait_chunk_sends((steps - 1) % 2, True)
    last_outs(steps - 1, 0, n_chunks - 1, True)
    finals = [pltpu.make_async_copy(h32.at[i], h_last.at[0, phys(i)], lsem.at[i]) for i in range(tile_h)]
    for copy in finals:
        copy.start()
    for slot in range(2):
        for i in range(tile_h):
            out_copy(0, slot, i).wait()
    for copy in finals:
        copy.wait()


def solution(mesh):
    n_rows, n_cols = mesh.shape["rows"], mesh.shape["cols"]
    frame_spec = P(None, "batch", "rows", "cols", None)
    state_spec = P("batch", "rows", "cols", None)

    def local_fn(frames, h_init, w_x, w_hzr, w_hn, gate_bias):
        steps, _, tile_h, tile_w, cin = frames.shape
        ch = h_init.shape[-1]
        dims = (steps, tile_h, tile_w, cin, ch)
        vm = pltpu.VMEM
        dma = pltpu.SemaphoreType.DMA
        kk = len(CHUNKS)
        wide = tile_w + 2 * COL_HALO
        scratch = [
            vm((3, 3, ch, 2 * ch), BF16), vm((3, 3, ch, ch), BF16), vm((256, 3 * ch), BF16), vm((3 * ch,), F32),
            vm((tile_h, steps, cin, tile_w), BF16), vm((tile_h + 4, wide, LANES), BF16),
            vm((2, 3, tile_h + 4, tile_w, ch), BF16), vm((3, tile_h + 2, tile_w, ch), BF16),
            vm((2, tile_h + 2, tile_w, ch), BF16), vm((2, kk, 16, ch), BF16), vm((8 * wide, LANES), F32),
            vm((tile_h, tile_w, ch), F32), vm((max(CHUNKS) * tile_w, ch), F32),
            vm((2, 2, tile_w, ch), F32), vm((2, 2, tile_w, ch), F32),
            vm((2, kk, 2, 16, ch), F32), vm((2, 2, kk, 16, ch), F32), vm((2, 4, 16, ch), F32), vm((6, 48, ch), F32),
            dma((3, tile_h)), dma((14,)), dma((14,)), dma((2, 2, kk)), dma((2, 2, kk)), dma((2, 4)), dma((2, 4)),
            dma((2,)), dma((2, 2)), dma((2, tile_h)), dma((tile_h,)),
        ]

        def body(*refs):
            kernel_body(n_cols, n_rows, dims, *refs)

        return pl.pallas_call(
            body,
            out_shape=(jax.ShapeDtypeStruct((steps, 1, tile_h, tile_w, ch), BF16), jax.ShapeDtypeStruct((1, tile_h, tile_w, ch), F32)),
            in_specs=[pl.BlockSpec(memory_space=pl.ANY)] * 6,
            out_specs=(pl.BlockSpec(memory_space=pl.ANY),) * 2,
            scratch_shapes=scratch,
            compiler_params=pltpu.CompilerParams(collective_id=0, has_side_effects=True, vmem_limit_bytes=56 * 1024 * 1024),
            name="convgru",
        )(jnp.swapaxes(frames, 3, 4), h_init, w_x, w_hzr, w_hn, gate_bias)

    return jax.shard_map(local_fn, mesh=mesh, in_specs=(frame_spec, state_spec, P(), P(), P(), P()), out_specs=(frame_spec, state_spec), check_vma=False)
```

```python
import jax
import jax.numpy as jnp
from jax import lax
from jax.experimental import pallas as pl
from jax.experimental.pallas import tpu as pltpu
from jax.sharding import PartitionSpec as P

BF16 = jnp.bfloat16
F32 = jnp.float32
MESH = pl.DeviceIdType.MESH
LANES = 128
COL_HALO = 16
CHUNKS = (6,) * 4
UNROLL = 2
VMEM_LIMIT = 40 * 1024 * 1024
NAMES = ("batch", "cols", "rows")


def sigmoid(v):
    return 0.5 * jnp.tanh(0.5 * v) + 0.5


def kernel_body(n_cols, n_rows, dims, frames, h_init, w_x, w_hzr, w_hn, bias, h_seq, h_last,
                wzr, wn, wx, bv, fv, fp, hb, rb, xp, xe, af, h32, zb, hf, hl, cs, cr, kr, cb,
                load_sem, fsend, frecv, csend, crecv, ksend, krecv, vsend, vrecv):
    steps, tile_h, tile_w, cin, ch = dims
    batch = lax.axis_index("batch")
    col = lax.axis_index("cols")
    row = lax.axis_index("rows")
    flip = lax.rem(row, 2)
    first_row = row - 1 + 2 * flip
    last_row = row + 1 - 2 * flip
    has_first = jnp.logical_and(first_row >= 0, first_row < n_rows)
    has_last = jnp.logical_and(last_row >= 0, last_row < n_rows)
    has_left = col > 0
    has_right = col < n_cols - 1
    both = jnp.logical_and
    left_dev = (batch, col - 1, row)
    right_dev = (batch, col + 1, row)
    first_dev = (batch, col, first_row)
    last_dev = (batch, col, last_row)
    corner_ok = (both(has_first, has_left), both(has_first, has_right), both(has_last, has_left), both(has_last, has_right))
    corner_dev = ((batch, col - 1, first_row), (batch, col + 1, first_row), (batch, col - 1, last_row), (batch, col + 1, last_row))
    around = ((has_left, left_dev), (has_right, right_dev), (has_first, first_dev), (has_last, last_dev)) + tuple(zip(corner_ok, corner_dev))

    def phys(i):
        return i + flip * (tile_h - 1 - 2 * i)

    n_chunks = len(CHUNKS)
    starts = [sum(CHUNKS[:k]) for k in range(n_chunks)]
    n_ranges = [(starts[k], CHUNKS[k]) for k in range(n_chunks)]
    r_ranges = []
    for k in range(n_chunks):
        lo = -1 if k == 0 else starts[k] + 1
        hi = tile_h + 1 if k == n_chunks - 1 else starts[k] + CHUNKS[k] + 1
        r_ranges.append((lo, hi - lo))

    def remote(src, dst, s_sem, r_sem, dev):
        return pltpu.make_async_remote_copy(src_ref=src, dst_ref=dst, send_sem=s_sem, recv_sem=r_sem, device_id=dev, device_id_type=MESH)

    loads = []
    for i in range(tile_h):
        loads.append(pltpu.make_async_copy(h_init.at[0, phys(i)], h32.at[i], load_sem.at[0, i]))
    frame_loads = [pltpu.make_async_copy(frames.at[:, 0, phys(i)], fv.at[i], load_sem.at[1, i]) for i in range(tile_h)]
    weight_loads = []
    for a in range(3):
        la = a + flip * (2 - 2 * a)
        weight_loads.append(pltpu.make_async_copy(w_hzr.at[a], wzr.at[la], load_sem.at[2, a]))
        weight_loads.append(pltpu.make_async_copy(w_hn.at[a], wn.at[la], load_sem.at[2, 3 + a]))
        for c in range(3):
            dst = wx.at[pl.ds(pl.multiple_of(64 * c + cin * la, cin), cin)]
            weight_loads.append(pltpu.make_async_copy(w_x.at[a, c], dst, load_sem.at[2, 6 + 3 * a + c]))
    weight_loads.append(pltpu.make_async_copy(bias, bv, load_sem.at[2, 15]))
    for copy in frame_loads + loads + weight_loads:
        copy.start()

    hf[...] = jnp.zeros_like(hf)
    hl[...] = jnp.zeros_like(hl)
    cr[...] = jnp.zeros_like(cr)
    kr[...] = jnp.zeros_like(kr)
    cb[...] = jnp.zeros_like(cb)
    cs[...] = jnp.zeros_like(cs)
    fp[...] = jnp.zeros_like(fp)
    for lo, hi in ((48, 64), (112, 128), (176, 256)):
        wx[lo:hi] = jnp.zeros((hi - lo, 3 * ch), BF16)

    barrier = pltpu.get_barrier_semaphore()
    count = 0
    for ok, dev in around:
        count = count + ok.astype(jnp.int32)

        @pl.when(ok)
        def _(dev=dev):
            pl.semaphore_signal(barrier, inc=1, device_id=dev, device_id_type=MESH)
    pl.semaphore_wait(barrier, count)

    lane = lax.broadcasted_iota(jnp.int32, (1, LANES), 1)

    for copy in frame_loads:
        copy.wait()
    own_c = pl.ds(COL_HALO, tile_w)
    for i in range(tile_h):
        fp[i + 2, own_c] = fv[i].reshape(steps * cin, tile_w).astype(F32).T.astype(BF16)

    lo_c = pl.ds(0, COL_HALO)
    hi_c = pl.ds(COL_HALO + tile_w, COL_HALO)
    own_lo = pl.ds(COL_HALO, COL_HALO)
    own_hi = pl.ds(tile_w, COL_HALO)
    f_copies = []
    own_r = pl.ds(2, tile_h)
    f_copies.append((has_left, fp.at[own_r, own_lo], fp.at[own_r, hi_c], left_dev))
    f_copies.append((has_right, fp.at[own_r, own_hi], fp.at[own_r, lo_c], right_dev))
    for ok, okl, okr, dev, cdl, cdr, rows in (
            (has_first, corner_ok[0], corner_ok[1], first_dev, corner_dev[0], corner_dev[1], ((2, 1), (3, 0))),
            (has_last, corner_ok[2], corner_ok[3], last_dev, corner_dev[2], corner_dev[3], ((tile_h + 1, tile_h + 2), (tile_h, tile_h + 3)))):
        for src, dst in rows:
            f_copies.append((ok, fp.at[src, own_c], fp.at[dst, own_c], dev))
            f_copies.append((okl, fp.at[src, own_lo], fp.at[dst, hi_c], cdl))
            f_copies.append((okr, fp.at[src, own_hi], fp.at[dst, lo_c], cdr))
    f_recv_index = [1, 0]
    for g in range(4):
        f_recv_index += [2 + 3 * g, 4 + 3 * g, 3 + 3 * g]
    f_descs = [(ok, remote(s, d, fsend.at[m], frecv.at[f_recv_index[m]], dev)) for m, (ok, s, d, dev) in enumerate(f_copies)]
    for ok, copy in f_descs:
        @pl.when(ok)
        def _(copy=copy):
            copy.start()

    def chunk_sends(k, slot):
        to_left = cs.at[slot, k, 0]
        to_right = cs.at[slot, k, 1]
        out = [(has_left, remote(to_left, cr.at[slot, 1, k], csend.at[slot, 0, k], crecv.at[slot, 1, k], left_dev)),
               (has_right, remote(to_right, cr.at[slot, 0, k], csend.at[slot, 1, k], crecv.at[slot, 0, k], right_dev))]
        for edge, q in ((0, 0), (n_chunks - 1, 2)):
            if k == edge:
                out.append((corner_ok[q], remote(to_left, kr.at[slot, q + 1], ksend.at[slot, q], krecv.at[slot, q + 1], corner_dev[q])))
                out.append((corner_ok[q + 1], remote(to_right, kr.at[slot, q], ksend.at[slot, q + 1], krecv.at[slot, q], corner_dev[q + 1])))
        return out

    def row_send(k, slot):
        if k == 0:
            return has_first, remote(h32.at[pl.ds(0, 2)], hf.at[slot], vsend.at[0], vrecv.at[slot, 0], first_dev)
        return has_last, remote(h32.at[pl.ds(tile_h - 2, 2)], hl.at[slot], vsend.at[1], vrecv.at[slot, 1], last_dev)

    def start_sends(k, slot, more):
        copies = chunk_sends(k, slot)
        if k in (0, n_chunks - 1):
            copies.append(row_send(k, slot))
        for ok, copy in copies:
            @pl.when(both(ok, more))
            def _(copy=copy):
                copy.start()

    def wait_chunk_sends(slot, cond):
        for k in range(n_chunks):
            for ok, copy in chunk_sends(k, slot):
                @pl.when(both(ok, cond))
                def _(copy=copy):
                    copy.wait_send()

    def wait_row_send(k, slot):
        ok, copy = row_send(k, slot)

        @pl.when(ok)
        def _():
            copy.wait_send()

    def wait_if(ok, dst, sem, src):
        @pl.when(ok)
        def _():
            remote(src, dst, csend.at[0, 0, 0], sem, right_dev).wait_recv()

    sub48 = lax.broadcasted_iota(jnp.int32, (tile_w, ch), 0)
    sub16 = lax.broadcasted_iota(jnp.int32, (16, ch), 0)

    def row_of(colbuf, i):
        return cb[colbuf, pl.ds(i + 8, 1), :]

    def publish(slot, i, v, k):
        hb[slot, 1, i + 2] = v.astype(BF16)
        hb[slot, 0, i + 2] = pltpu.roll(v, 1, 0).astype(BF16)
        hb[slot, 2, i + 2] = pltpu.roll(v, tile_w - 1, 0).astype(BF16)
        j = i - starts[k]
        for side, m, x in ((0, 0, 0), (0, 1, 1), (1, 0, tile_w - 2), (1, 1, tile_w - 1)):
            cs[slot, k, side, pl.ds(8 * m + j, 1), :] = v[x:x + 1]
        cb[2, pl.ds(i + 8, 1), :] = v[0:1]
        cb[3, pl.ds(i + 8, 1), :] = v[tile_w - 1:tile_w]

    def wait_cols(slot, k):
        wait_if(has_left, cr.at[slot, 0, k], crecv.at[slot, 0, k], cs.at[slot, k, 0])
        wait_if(has_right, cr.at[slot, 1, k], crecv.at[slot, 1, k], cs.at[slot, k, 0])

    def place_cols(slot, k):
        i0, n = n_ranges[k]
        for side in range(2):
            for m in range(2):
                cb[4 * side + m, pl.ds(i0 + 8, n), :] = cr[slot, side, k, 8 * m:8 * m + n, :]
        for i in range(i0, i0 + n):
            old = hb[slot, 0, i + 2, 0:16].astype(F32)
            hb[slot, 0, i + 2, 0:16] = jnp.where(sub16 == 0, row_of(1, i), old).astype(BF16)
            old = hb[slot, 2, i + 2, tile_w - 16:tile_w].astype(F32)
            hb[slot, 2, i + 2, tile_w - 16:tile_w] = jnp.where(sub16 == 15, row_of(4, i), old).astype(BF16)

    def wait_rows(slot, last):
        src, ok = (hl, has_last) if last else (hf, has_first)
        wait_if(ok, src.at[slot], vrecv.at[slot, last], h32.at[pl.ds(0, 2)])
        for m in range(2):
            q = 2 * last + m
            wait_if(corner_ok[q], kr.at[slot, q], krecv.at[slot, q], cs.at[slot, 0, 0])

    def place_rows(slot, last):
        src = hl if last else hf
        for depth in range(2):
            i = tile_h + depth if last else -1 - depth
            m = 1 - depth if last else depth
            j = CHUNKS[-1] - 1 - depth if last else depth
            for x in range(2):
                cb[x, pl.ds(i + 8, 1), :] = kr[slot, 2 * last, 8 * x + j:8 * x + j + 1, :]
                cb[4 + x, pl.ds(i + 8, 1), :] = kr[slot, 2 * last + 1, 8 * x + j:8 * x + j + 1, :]
            v = src[slot, m]
            cb[2, pl.ds(i + 8, 1), :] = v[0:1]
            cb[3, pl.ds(i + 8, 1), :] = v[tile_w - 1:tile_w]
            hb[slot, 1, i + 2] = v.astype(BF16)
            hb[slot, 0, i + 2] = jnp.where(sub48 == 0, row_of(1, i), pltpu.roll(v, 1, 0)).astype(BF16)
            hb[slot, 2, i + 2] = jnp.where(sub48 == tile_w - 1, row_of(4, i), pltpu.roll(v, tile_w - 1, 0)).astype(BF16)

    wide = tile_w + 2 * COL_HALO

    def build_x(t, slot, k):
        i0, n = r_ranges[k]
        for j in range(n):
            parts = [pltpu.roll(fp[i0 + j + a + 1].astype(F32), lax.rem(cin * a - cin * t + cin * steps, cin * steps), 1) for a in range(3)]
            af[pl.ds(j * wide, wide)] = jnp.where(lane < cin, parts[0], jnp.where(lane < 2 * cin, parts[1], parts[2]))
        for j in range(n):
            base = j * wide + COL_HALO
            left = af[pl.ds(base - 1, tile_w)]
            mid = pltpu.roll(af[pl.ds(base, tile_w)], 64, 1)
            xp[slot, i0 + j + 1, :, 0:LANES] = jnp.where(lane < 64, left, mid).astype(BF16)
            xp[slot, i0 + j + 1, :, LANES:2 * LANES] = af[pl.ds(base + 1, tile_w)].astype(BF16)
        lo_half, hi_half = [], []
        for x in (-1, tile_w):
            three = [af[pl.ds(COL_HALO + x + c - 1, 8, wide)] for c in range(3)]
            lo_half.append(jnp.where(lane < 64, three[0], pltpu.roll(three[1], 64, 1)))
            hi_half.append(three[2])
        xe[slot, k, :, 0:LANES] = jnp.concatenate(lo_half, axis=0).astype(BF16)
        xe[slot, k, :, LANES:2 * LANES] = jnp.concatenate(hi_half, axis=0).astype(BF16)

    def conv(src, i0, n, off, weights, xslot, gate, extra=None, e_lo=0):
        lo, w_lo = gate * ch, (0 if gate == 2 else gate * ch)
        acc = None
        for c in (1, 0, 2):
            for a in range(3):
                lhs = src(c, pl.ds(i0 + a - 1 - off, n)).reshape(n * tile_w, ch)
                if extra is not None:
                    ends = [cb[3 * side + c, pl.ds(e_lo + a - 1 + 8, 8), :] for side in range(2)]
                    lhs = jnp.concatenate([lhs, jnp.concatenate(ends, axis=0).astype(BF16)], axis=0)
                part = jnp.dot(lhs, weights[a, c, :, w_lo:w_lo + ch], preferred_element_type=F32)
                acc = part if acc is None else acc + part
        lhs = xp[xslot, pl.ds(i0 + 1, n)].reshape(n * tile_w, ch)
        if extra is not None:
            lhs = jnp.concatenate([lhs, xe[xslot, extra]], axis=0)
        acc = acc + jnp.dot(lhs, wx[:, lo:lo + ch], preferred_element_type=F32)
        return acc + bv[lo:lo + ch].reshape(1, ch)

    for copy in loads:
        copy.wait()
    for k in range(n_chunks):
        i0, n = n_ranges[k]
        for i in range(i0, i0 + n):
            publish(0, i, h32[i], k)
        start_sends(k, 0, True)
    for m, (ok, copy) in enumerate(f_descs):
        src, dst = f_copies[m][1], f_copies[f_recv_index[m]][2]

        @pl.when(ok)
        def _(copy=copy, m=m, src=src, dst=dst):
            copy.wait_send()
            remote(src, dst, fsend.at[m], frecv.at[m], right_dev).wait_recv()
    for k in range(n_chunks):
        build_x(0, 0, k)
    for copy in weight_loads:
        copy.wait()

    def halves(i0, n):
        return (i0, n - n // 2), (i0 + n - n // 2, n // 2)

    def meet(t, now, k):
        new = 1 - now
        if k == 0:
            start_sends(n_chunks - 1, now, both(t > 0, True))
            free_slot(t, now)
            wait_cols(now, 0)
            wait_rows(now, 0)
            wait_row_send(0, now)
        else:
            start_sends(k - 1, new, t < steps - 1)
        if k + 1 < n_chunks:
            wait_cols(now, k + 1)
        else:
            wait_rows(now, 1)
            wait_row_send(n_chunks - 1, now)
        if k == 0:
            place_cols(now, 0)
            place_rows(now, 0)
        if k + 1 < n_chunks:
            place_cols(now, k + 1)
        else:
            place_rows(now, 1)

    def free_slot(t, now):
        new = 1 - now
        wait_chunk_sends(new, t >= 1)

    def stretch(t, now, k):
        new = 1 - now
        meet(t, now, k)
        r_lo, r_n = r_ranges[k]
        parts = halves(r_lo, r_n)
        accs = [conv(lambda c, rows: hb[now, c, rows], i0, n, -2, wzr, now, 1, extra=k if h == 1 else None, e_lo=r_lo) for h, (i0, n) in enumerate(parts)]
        gates = [sigmoid(acc) for acc in accs]
        ends = gates[1][parts[1][1] * tile_w:]
        ends_l = ends[0:8] * cb[1, pl.ds(r_lo + 8, 8), :]
        ends_r = ends[8:16] * cb[4, pl.ds(r_lo + 8, 8), :]
        for (i0, n), gate in zip(parts, gates):
            for j in range(n):
                i = i0 + j
                e = i - r_lo
                old = hf[now, 0] if i == -1 else hl[now, 1] if i == tile_h else h32[i]
                v = gate[j * tile_w:(j + 1) * tile_w] * old
                rb[1, i + 1] = v.astype(BF16)
                rb[0, i + 1] = jnp.where(sub48 == 0, ends_l[e:e + 1], pltpu.roll(v, 1, 0)).astype(BF16)
                rb[2, i + 1] = jnp.where(sub48 == tile_w - 1, ends_r[e:e + 1], pltpu.roll(v, tile_w - 1, 0)).astype(BF16)
        parts = halves(*n_ranges[k])
        accs = [conv(lambda c, rows: hb[now, c, rows], i0, n, -2, wzr, now, 0) for i0, n in parts]
        for (i0, n), acc in zip(parts, accs):
            zb[pl.ds((i0 - n_ranges[k][0]) * tile_w, n * tile_w)] = sigmoid(acc)
        build_x(jnp.minimum(t + 1, steps - 1), new, k)
        accs = [conv(lambda c, rows: rb[c, rows], i0, n, -1, wn, now, 2) for i0, n in parts]
        for (i0, n), acc in zip(parts, accs):
            cand = jnp.tanh(acc)
            for j in range(n):
                i = i0 + j
                mix = cand[j * tile_w:(j + 1) * tile_w]
                v = mix + zb[pl.ds((i - n_ranges[k][0]) * tile_w, tile_w)] * (h32[i] - mix)
                h32[i] = v
                h_seq[t, 0, phys(i)] = v.astype(BF16)
                publish(new, i, v, k)

    def body(p, carry):
        for s in range(UNROLL):
            for k in range(n_chunks):
                stretch(UNROLL * p + s, s % 2, k)
        return carry

    lax.fori_loop(0, steps // UNROLL, body, 0)
    wait_chunk_sends((steps - 1) % 2, True)
    for i in range(tile_h):
        h_last[0, phys(i)] = h32[i]


def solution(mesh):
    n_rows, n_cols = mesh.shape["rows"], mesh.shape["cols"]
    frame_spec = P(None, "batch", "rows", "cols", None)
    state_spec = P("batch", "rows", "cols", None)

    def local_fn(frames, h_init, w_x, w_hzr, w_hn, gate_bias):
        steps, _, tile_h, tile_w, cin = frames.shape
        ch = h_init.shape[-1]
        dims = (steps, tile_h, tile_w, cin, ch)
        vm = pltpu.VMEM
        dma = pltpu.SemaphoreType.DMA
        kk = len(CHUNKS)
        wide = tile_w + 2 * COL_HALO
        scratch = [
            vm((3, 3, ch, 2 * ch), BF16), vm((3, 3, ch, ch), BF16), vm((256, 3 * ch), BF16), vm((3 * ch,), F32),
            vm((tile_h, steps, cin, tile_w), BF16), vm((tile_h + 4, wide, LANES), BF16),
            vm((2, 3, tile_h + 4, tile_w, ch), BF16), vm((3, tile_h + 2, tile_w, ch), BF16),
            vm((2, tile_h + 2, tile_w, ch), BF16), vm((2, kk, 16, ch), BF16), vm((8 * wide, LANES), F32),
            vm((tile_h, tile_w, ch), F32), vm((max(CHUNKS) * tile_w, ch), F32),
            vm((2, 2, tile_w, ch), F32), vm((2, 2, tile_w, ch), F32),
            vm((2, kk, 2, 16, ch), F32), vm((2, 2, kk, 16, ch), F32), vm((2, 4, 16, ch), F32), vm((6, 48, ch), F32),
            dma((3, tile_h)), dma((14,)), dma((14,)), dma((2, 2, kk)), dma((2, 2, kk)), dma((2, 4)), dma((2, 4)),
            dma((2,)), dma((2, 2)),
        ]

        def body(*refs):
            kernel_body(n_cols, n_rows, dims, *refs)

        return pl.pallas_call(
            body,
            out_shape=(vm((steps, 1, tile_h, tile_w, ch), BF16), vm((1, tile_h, tile_w, ch), F32)),
            in_specs=[pl.BlockSpec(memory_space=pltpu.HBM)] * 6,
            out_specs=(pl.BlockSpec(memory_space=vm),) * 2,
            scratch_shapes=scratch,
            compiler_params=pltpu.CompilerParams(collective_id=0, has_side_effects=True, vmem_limit_bytes=VMEM_LIMIT),
            name="convgru",
        )(*[pltpu.with_memory_space_constraint(v, pltpu.HBM) for v in (jnp.swapaxes(frames, 3, 4), h_init, w_x, w_hzr, w_hn, gate_bias)])

    return jax.shard_map(local_fn, mesh=mesh, in_specs=(frame_spec, state_spec, P(), P(), P(), P()), out_specs=(frame_spec, state_spec), check_vma=False)
```

```python
import jax
import jax.numpy as jnp
from jax import lax
from jax.experimental import pallas as pl
from jax.experimental.pallas import tpu as pltpu
from jax.sharding import PartitionSpec as P

BF16 = jnp.bfloat16
F32 = jnp.float32
MESH = pl.DeviceIdType.MESH
LANES = 128
COL_HALO = 8
CHUNKS = (6,) * 4
UNROLL = 2
AHEAD = 5
VMEM_LIMIT = 40 * 1024 * 1024
NAMES = ("batch", "cols", "rows")


def sigmoid(v):
    return 0.5 * jnp.tanh(0.5 * v) + 0.5


def kernel_body(n_cols, n_rows, dims, frames, h_init, w_x, w_hzr, w_hn, bias, h_seq, h_last,
                wzr, wn, wx, bv, fv, fp, fcs, fcr, fkr, hb, rb, xp, xe, af, hraw, h32, zb, hf, hl, cs, cr, kr, cb,
                load_sem, fsend, frecv, csend, crecv, ksend, krecv, vsend, vrecv):
    steps, tile_h, tile_w, cin, ch = dims
    edge_cells = ((0, 0, 0), (0, 1, 1), (1, 0, tile_w - 2), (1, 1, tile_w - 1))
    batch = lax.axis_index("batch")
    col = lax.axis_index("cols")
    row = lax.axis_index("rows")
    flip = lax.rem(row, 2)
    first_row = row - 1 + 2 * flip
    last_row = row + 1 - 2 * flip
    has_first = jnp.logical_and(first_row >= 0, first_row < n_rows)
    has_last = jnp.logical_and(last_row >= 0, last_row < n_rows)
    has_left = col > 0
    has_right = col < n_cols - 1
    both = jnp.logical_and
    left_dev = (batch, col - 1, row)
    right_dev = (batch, col + 1, row)
    first_dev = (batch, col, first_row)
    last_dev = (batch, col, last_row)
    corner_ok = (both(has_first, has_left), both(has_first, has_right), both(has_last, has_left), both(has_last, has_right))
    corner_dev = ((batch, col - 1, first_row), (batch, col + 1, first_row), (batch, col - 1, last_row), (batch, col + 1, last_row))
    around = ((has_left, left_dev), (has_right, right_dev), (has_first, first_dev), (has_last, last_dev)) + tuple(zip(corner_ok, corner_dev))

    def phys(i):
        return i + flip * (tile_h - 1 - 2 * i)

    n_chunks = len(CHUNKS)
    starts = [sum(CHUNKS[:k]) for k in range(n_chunks)]
    n_ranges = [(starts[k], CHUNKS[k]) for k in range(n_chunks)]
    r_ranges = []
    for k in range(n_chunks):
        lo = -1 if k == 0 else starts[k] + 1
        hi = tile_h + 1 if k == n_chunks - 1 else starts[k] + CHUNKS[k] + 1
        r_ranges.append((lo, hi - lo))

    def remote(src, dst, s_sem, r_sem, dev):
        return pltpu.make_async_remote_copy(src_ref=src, dst_ref=dst, send_sem=s_sem, recv_sem=r_sem, device_id=dev, device_id_type=MESH)

    def chunk_rows(k):
        i0, n = n_ranges[k]
        return pl.ds(i0 + flip * (tile_h - n - 2 * i0), n)

    loads = [pltpu.make_async_copy(h_init.at[0, chunk_rows(k)], hraw.at[chunk_rows(k)], load_sem.at[0, k]) for k in range(n_chunks)]
    frame_loads = [pltpu.make_async_copy(frames.at[:, 0], fv, load_sem.at[1, 0])]
    weight_loads = []
    for a in range(3):
        la = a + flip * (2 - 2 * a)
        weight_loads.append(pltpu.make_async_copy(w_hzr.at[a], wzr.at[la], load_sem.at[2, a]))
        weight_loads.append(pltpu.make_async_copy(w_hn.at[a], wn.at[la], load_sem.at[2, 3 + a]))
        for c in range(3):
            dst = wx.at[pl.ds(pl.multiple_of(64 * c + cin * la, cin), cin)]
            weight_loads.append(pltpu.make_async_copy(w_x.at[a, c], dst, load_sem.at[2, 6 + 3 * a + c]))
    weight_loads.append(pltpu.make_async_copy(bias, bv, load_sem.at[2, 15]))
    for copy in loads + frame_loads + weight_loads:
        copy.start()

    hf[...] = jnp.zeros_like(hf)
    hl[...] = jnp.zeros_like(hl)
    cr[...] = jnp.zeros_like(cr)
    kr[...] = jnp.zeros_like(kr)
    cb[...] = jnp.zeros_like(cb)
    fcr[...] = jnp.zeros_like(fcr)
    fkr[...] = jnp.zeros_like(fkr)
    for i in (0, 1, tile_h + 2, tile_h + 3):
        fp[i] = jnp.zeros_like(fp[i])
    for lo in (0, COL_HALO + tile_w):
        fp[:, lo:lo + COL_HALO, :] = jnp.zeros((tile_h + 4, COL_HALO, LANES), F32)
    for lo, hi in ((48, 64), (112, 128), (176, 256)):
        wx[lo:hi] = jnp.zeros((hi - lo, 3 * ch), BF16)

    barrier = pltpu.get_barrier_semaphore()
    count = 0
    for ok, dev in around:
        count = count + ok.astype(jnp.int32)

        @pl.when(ok)
        def _(dev=dev):
            pl.semaphore_signal(barrier, inc=1, device_id=dev, device_id_type=MESH)
    lane = lax.broadcasted_iota(jnp.int32, (1, LANES), 1)

    own_c = pl.ds(COL_HALO, tile_w)

    def pack_frames():
        for i in range(tile_h):
            v = fv[:, phys(i)].reshape(steps * cin, tile_w).astype(F32).T
            fp[i + 2, own_c] = v
            for side, m, x in edge_cells:
                fcs[side, m, pl.ds(i, 1), :] = v[x:x + 1]

    def frame_copies():
        out = [(has_left, remote(fcs.at[0], fcr.at[1], fsend.at[0], frecv.at[1], left_dev), fcr.at[0], frecv.at[0]),
               (has_right, remote(fcs.at[1], fcr.at[0], fsend.at[1], frecv.at[0], right_dev), fcr.at[1], frecv.at[1])]
        rows = ((has_first, first_dev, 2, 1), (has_first, first_dev, 3, 0), (has_last, last_dev, tile_h + 1, tile_h + 2), (has_last, last_dev, tile_h, tile_h + 3))
        for m, (ok, dev, src, dst) in enumerate(rows):
            out.append((ok, remote(fp.at[src, own_c], fp.at[dst, own_c], fsend.at[2 + m], frecv.at[2 + m], dev), fp.at[dst, own_c], frecv.at[2 + m]))
        for q in range(4):
            near = pl.ds(0 if q < 2 else tile_h - 8, 8)
            other = q ^ 1
            out.append((corner_ok[q], remote(fcs.at[q % 2, :, near], fkr.at[other], fsend.at[6 + q], frecv.at[6 + other], corner_dev[q]), fkr.at[q], frecv.at[6 + q]))
        return out

    def place_frames():
        for i in range(tile_h):
            for side, base in ((0, COL_HALO - 2), (1, COL_HALO + tile_w)):
                for m in range(2):
                    fp[i + 2, pl.ds(base + m, 1), :] = fcr[side, m, i:i + 1, :]
        for q in range(4):
            base = COL_HALO - 2 if q % 2 == 0 else COL_HALO + tile_w
            for depth in range(2):
                i = -1 - depth if q < 2 else tile_h + depth
                j = depth if q < 2 else 7 - depth
                for m in range(2):
                    fp[i + 2, pl.ds(base + m, 1), :] = fkr[q, m, j:j + 1, :]

    def chunk_sends(k, slot):
        to_left = cs.at[slot, 0, k]
        to_right = cs.at[slot, 1, k]
        out = [(has_left, remote(to_left, cr.at[slot, 1, k], csend.at[slot, 0], crecv.at[slot, 1, k], left_dev)),
               (has_right, remote(to_right, cr.at[slot, 0, k], csend.at[slot, 1], crecv.at[slot, 0, k], right_dev))]
        for edge, q in ((0, 0), (n_chunks - 1, 2)):
            if k == edge:
                out.append((corner_ok[q], remote(to_left, kr.at[slot, q + 1], ksend.at[slot, q], krecv.at[slot, q + 1], corner_dev[q])))
                out.append((corner_ok[q + 1], remote(to_right, kr.at[slot, q], ksend.at[slot, q + 1], krecv.at[slot, q], corner_dev[q + 1])))
        return out

    def row_send(k, slot):
        if k == 0:
            return has_first, remote(h32.at[pl.ds(0, 2)], hf.at[slot], vsend.at[0], vrecv.at[slot, 0], first_dev)
        return has_last, remote(h32.at[pl.ds(tile_h - 2, 2)], hl.at[slot], vsend.at[1], vrecv.at[slot, 1], last_dev)

    def start_sends(k, slot, more):
        copies = chunk_sends(k, slot)
        if k in (0, n_chunks - 1):
            copies.append(row_send(k, slot))
        for ok, copy in copies:
            @pl.when(both(ok, more))
            def _(copy=copy):
                copy.start()

    def wait_chunk_sends(slot, cond):
        copies = [(ok, remote(cs.at[slot, m], cr.at[slot, m], csend.at[slot, m], csend.at[slot, m], dev))
                  for m, (ok, dev) in enumerate(((has_left, left_dev), (has_right, right_dev)))]
        copies += chunk_sends(0, slot)[2:] + chunk_sends(n_chunks - 1, slot)[2:]
        for ok, copy in copies:
            @pl.when(both(ok, cond))
            def _(copy=copy):
                copy.wait_send()

    def wait_row_send(k, slot):
        ok, copy = row_send(k, slot)

        @pl.when(ok)
        def _():
            copy.wait_send()

    def wait_if(ok, dst, sem, src):
        @pl.when(ok)
        def _():
            remote(src, dst, csend.at[0, 0], sem, right_dev).wait_recv()

    sub48 = lax.broadcasted_iota(jnp.int32, (tile_w, ch), 0)
    sub16 = lax.broadcasted_iota(jnp.int32, (16, ch), 0)

    def row_of(colbuf, i):
        return cb[colbuf, pl.ds(i + 8, 1), :]

    def publish(slot, i, v, k):
        hb[slot, 1, i + 2] = v.astype(BF16)
        hb[slot, 0, i + 2] = pltpu.roll(v, 1, 0).astype(BF16)
        hb[slot, 2, i + 2] = pltpu.roll(v, tile_w - 1, 0).astype(BF16)
        j = i - starts[k]
        for side, m, x in edge_cells:
            cs[slot, side, k, pl.ds(8 * m + j, 1), :] = v[x:x + 1]
        cb[2, pl.ds(i + 8, 1), :] = v[0:1]
        cb[3, pl.ds(i + 8, 1), :] = v[tile_w - 1:tile_w]

    def wait_cols(slot, k):
        wait_if(has_left, cr.at[slot, 0, k], crecv.at[slot, 0, k], cs.at[slot, 0, k])
        wait_if(has_right, cr.at[slot, 1, k], crecv.at[slot, 1, k], cs.at[slot, 0, k])

    def place_cols(slot, k):
        i0, n = n_ranges[k]
        for side in range(2):
            for m in range(2):
                cb[4 * side + m, pl.ds(i0 + 8, n), :] = cr[slot, side, k, 8 * m:8 * m + n, :]
        for i in range(i0, i0 + n):
            old = hb[slot, 0, i + 2, 0:16].astype(F32)
            hb[slot, 0, i + 2, 0:16] = jnp.where(sub16 == 0, row_of(1, i), old).astype(BF16)
            old = hb[slot, 2, i + 2, tile_w - 16:tile_w].astype(F32)
            hb[slot, 2, i + 2, tile_w - 16:tile_w] = jnp.where(sub16 == 15, row_of(4, i), old).astype(BF16)

    def wait_rows(slot, last):
        src, ok = (hl, has_last) if last else (hf, has_first)
        wait_if(ok, src.at[slot], vrecv.at[slot, last], h32.at[pl.ds(0, 2)])
        for m in range(2):
            q = 2 * last + m
            wait_if(corner_ok[q], kr.at[slot, q], krecv.at[slot, q], cs.at[slot, 0, 0])

    def place_rows(slot, last):
        src = hl if last else hf
        for depth in range(2):
            i = tile_h + depth if last else -1 - depth
            m = 1 - depth if last else depth
            j = CHUNKS[-1] - 1 - depth if last else depth
            for x in range(2):
                cb[x, pl.ds(i + 8, 1), :] = kr[slot, 2 * last, 8 * x + j:8 * x + j + 1, :]
                cb[4 + x, pl.ds(i + 8, 1), :] = kr[slot, 2 * last + 1, 8 * x + j:8 * x + j + 1, :]
            v = src[slot, m]
            cb[2, pl.ds(i + 8, 1), :] = v[0:1]
            cb[3, pl.ds(i + 8, 1), :] = v[tile_w - 1:tile_w]
            hb[slot, 1, i + 2] = v.astype(BF16)
            hb[slot, 0, i + 2] = jnp.where(sub48 == 0, row_of(1, i), pltpu.roll(v, 1, 0)).astype(BF16)
            hb[slot, 2, i + 2] = jnp.where(sub48 == tile_w - 1, row_of(4, i), pltpu.roll(v, tile_w - 1, 0)).astype(BF16)

    wide = tile_w + 2 * COL_HALO

    def build_x(t, k):
        i0, n = r_ranges[k]
        for j in range(n):
            parts = [pltpu.roll(fp[i0 + j + a + 1], lax.rem(cin * a - cin * t + cin * steps, cin * steps), 1) for a in range(3)]
            af[pl.ds(j * wide, wide)] = jnp.where(lane < cin, parts[0], jnp.where(lane < 2 * cin, parts[1], parts[2]))
        for j in range(n):
            base = j * wide + COL_HALO
            left = af[pl.ds(base - 1, tile_w)]
            mid = pltpu.roll(af[pl.ds(base, tile_w)], 64, 1)
            xp[i0 + j + 1, :, 0:LANES] = jnp.where(lane < 64, left, mid).astype(BF16)
            xp[i0 + j + 1, :, LANES:2 * LANES] = af[pl.ds(base + 1, tile_w)].astype(BF16)
        lo_half, hi_half = [], []
        for x in (-1, tile_w):
            three = [af[pl.ds(COL_HALO + x + c - 1, 8, wide)] for c in range(3)]
            lo_half.append(jnp.where(lane < 64, three[0], pltpu.roll(three[1], 64, 1)))
            hi_half.append(three[2])
        xe[k, :, 0:LANES] = jnp.concatenate(lo_half, axis=0).astype(BF16)
        xe[k, :, LANES:2 * LANES] = jnp.concatenate(hi_half, axis=0).astype(BF16)

    all_taps = ["x"] + [(a, c) for c in (1, 0, 2) for a in range(3)]

    def conv(src, i0, n, off, weights, gate, extra=None, e_lo=0, taps=all_taps, acc=None):
        lo, w_lo = gate * ch, (0 if gate == 2 else gate * ch)
        for tap in taps:
            if tap == "x":
                lhs = xp[pl.ds(i0 + 1, n)].reshape(n * tile_w, ch)
                more = None if extra is None else xe[extra]
                weight = wx[:, lo:lo + ch]
            else:
                a, c = tap
                lhs = src(c, pl.ds(i0 + a - 1 - off, n)).reshape(n * tile_w, ch)
                more = None if extra is None else jnp.concatenate(
                    [cb[3 * side + c, pl.ds(e_lo + a - 1 + 8, 8), :] for side in range(2)], axis=0).astype(BF16)
                weight = weights[a, c, :, w_lo:w_lo + ch]
            if more is not None:
                lhs = jnp.concatenate([lhs, more], axis=0)
            part = jnp.dot(lhs, weight, preferred_element_type=F32)
            acc = part if acc is None else acc + part
        return acc

    def biased(acc, gate):
        return acc + bv[gate * ch:(gate + 1) * ch].reshape(1, ch)

    for k in range(n_chunks):
        loads[k].wait()
    for k in range(n_chunks):
        i0, n = n_ranges[k]
        for i in range(i0, i0 + n):
            v = hraw[phys(i)]
            h32[i] = v
            publish(0, i, v, k)
    for copy in frame_loads:
        copy.wait()
    pl.semaphore_wait(barrier, count)
    for k in range(n_chunks):
        start_sends(k, 0, True)
    pack_frames()
    f_descs = frame_copies()
    for ok, copy, _, _ in f_descs:
        @pl.when(ok)
        def _(copy=copy):
            copy.start()
    for ok, copy, _, _ in f_descs:
        @pl.when(ok)
        def _(copy=copy):
            copy.wait_send()
    for copy in weight_loads:
        copy.wait()
    for ok, copy, dst, sem in f_descs:
        @pl.when(ok)
        def _(dst=dst, sem=sem):
            remote(dst, dst, fsend.at[0], sem, right_dev).wait_recv()
    place_frames()
    build_x(0, 0)

    def halves(i0, n):
        return (i0, n - n // 2), (i0 + n - n // 2, n // 2)

    def meet(t, now, k):
        new = 1 - now
        if k == 0:
            start_sends(n_chunks - 1, now, both(t > 0, True))
            free_slot(t, now)
            wait_cols(now, 0)
            wait_rows(now, 0)
            wait_row_send(0, now)
        else:
            start_sends(k - 1, new, t < steps - 1)
        if k + 1 < n_chunks:
            wait_cols(now, k + 1)
        else:
            wait_rows(now, 1)
            wait_row_send(n_chunks - 1, now)
        if k == 0:
            place_cols(now, 0)
            place_rows(now, 0)
        if k + 1 < n_chunks:
            place_cols(now, k + 1)
        else:
            place_rows(now, 1)

    def free_slot(t, now):
        new = 1 - now
        wait_chunk_sends(new, t >= 1)

    def ahead(now, k):
        out = []
        for h, (i0, n) in enumerate(halves(*n_ranges[k])):
            skip = 0 if k == 0 and h == 0 else 2 if k == n_chunks - 1 and h == 1 else None
            taps = [tap for tap in all_taps if tap == "x" or tap[0] != skip and (tap[1] == 1 or k > 0 and tap[0] < 2)][:AHEAD]
            acc = conv(lambda c, rows: hb[now, c, rows], i0, n, -2, wzr, 0, taps=taps)
            out.append((taps, acc))
        return out

    def stretch(t, now, k, begun, carry_on):
        new = 1 - now
        meet(t, now, k)
        r_lo, r_n = r_ranges[k]
        parts = halves(r_lo, r_n)
        accs = [conv(lambda c, rows: hb[now, c, rows], i0, n, -2, wzr, 1, extra=k if h == k % 2 else None, e_lo=r_lo) for h, (i0, n) in enumerate(parts)]
        gates = [sigmoid(biased(acc, 1)) for acc in accs]
        ends = gates[k % 2][parts[k % 2][1] * tile_w:]
        ends_l = ends[0:8] * cb[1, pl.ds(r_lo + 8, 8), :]
        ends_r = ends[8:16] * cb[4, pl.ds(r_lo + 8, 8), :]
        for (i0, n), gate in zip(parts, gates):
            for j in range(n):
                i = i0 + j
                e = i - r_lo
                old = hf[now, 0] if i == -1 else hl[now, 1] if i == tile_h else h32[i]
                v = gate[j * tile_w:(j + 1) * tile_w] * old
                rb[1, i + 1] = v.astype(BF16)
                rb[0, i + 1] = jnp.where(sub48 == 0, ends_l[e:e + 1], pltpu.roll(v, 1, 0)).astype(BF16)
                rb[2, i + 1] = jnp.where(sub48 == tile_w - 1, ends_r[e:e + 1], pltpu.roll(v, tile_w - 1, 0)).astype(BF16)
        parts = halves(*n_ranges[k])
        for h, (i0, n) in enumerate(parts):
            done, acc = begun[h] if begun is not None else ([], None)
            acc = conv(lambda c, rows: hb[now, c, rows], i0, n, -2, wzr, 0, taps=[tap for tap in all_taps if tap not in done], acc=acc)
            zb[pl.ds((i0 - n_ranges[k][0]) * tile_w, n * tile_w)] = sigmoid(biased(acc, 0))
        if k + 1 < n_chunks:
            build_x(t, k + 1)
        else:
            build_x(jnp.minimum(t + 1, steps - 1), 0)
        accs = [conv(lambda c, rows: rb[c, rows], i0, n, -1, wn, 2) for i0, n in parts]
        begun = None
        if carry_on and k + 1 < n_chunks:
            begun = ahead(now, k + 1)
        for (i0, n), acc in zip(parts, accs):
            cand = jnp.tanh(biased(acc, 2))
            for j in range(n):
                i = i0 + j
                mix = cand[j * tile_w:(j + 1) * tile_w]
                v = mix + zb[pl.ds((i - n_ranges[k][0]) * tile_w, tile_w)] * (h32[i] - mix)
                h32[i] = v
                h_seq[t, 0, phys(i)] = v.astype(BF16)
                publish(new, i, v, k)
        if carry_on and k + 1 == n_chunks:
            begun = ahead(new, 0)
        return begun

    def body(p, carry):
        begun = None
        for s in range(UNROLL):
            for k in range(n_chunks):
                last = s == UNROLL - 1 and k == n_chunks - 1
                begun = stretch(UNROLL * p + s, s % 2, k, begun, not last)
        return carry

    lax.fori_loop(0, steps // UNROLL, body, 0)
    wait_chunk_sends((steps - 1) % 2, True)
    for i in range(tile_h):
        h_last[0, phys(i)] = h32[i]


def solution(mesh):
    n_rows, n_cols = mesh.shape["rows"], mesh.shape["cols"]
    frame_spec = P(None, "batch", "rows", "cols", None)
    state_spec = P("batch", "rows", "cols", None)

    def local_fn(frames, h_init, w_x, w_hzr, w_hn, gate_bias):
        steps, _, tile_h, tile_w, cin = frames.shape
        ch = h_init.shape[-1]
        dims = (steps, tile_h, tile_w, cin, ch)
        vm = pltpu.VMEM
        dma = pltpu.SemaphoreType.DMA
        kk = len(CHUNKS)
        wide = tile_w + 2 * COL_HALO
        pair = (2, 2)
        scratch = [
            vm((3, 3, ch, 2 * ch), BF16), vm((3, 3, ch, ch), BF16), vm((256, 3 * ch), BF16), vm((3 * ch,), F32),
            vm((steps, tile_h, cin, tile_w), BF16), vm((tile_h + 4, wide, LANES), F32),
            vm(pair + (tile_h, LANES), F32), vm(pair + (tile_h, LANES), F32), vm((4, 2, 8, LANES), F32),
            vm((2, 3, tile_h + 4, tile_w, ch), BF16), vm((3, tile_h + 2, tile_w, ch), BF16),
            vm((tile_h + 2, tile_w, ch), BF16), vm((kk, 16, ch), BF16), vm((8 * wide, LANES), F32),
            vm((tile_h, tile_w, ch), F32), vm((tile_h, tile_w, ch), F32), vm((max(CHUNKS) * tile_w, ch), F32),
            vm(pair + (tile_w, ch), F32), vm(pair + (tile_w, ch), F32),
            vm(pair + (kk, 16, ch), F32), vm(pair + (kk, 16, ch), F32), vm((2, 4, 16, ch), F32), vm((6, 48, ch), F32),
            dma((3, tile_h)), dma((10,)), dma((10,)), dma(pair), dma(pair + (kk,)), dma((2, 4)), dma((2, 4)),
            dma((2,)), dma(pair),
        ]

        def body(*refs):
            kernel_body(n_cols, n_rows, dims, *refs)

        return pl.pallas_call(
            body,
            out_shape=(vm((steps, 1, tile_h, tile_w, ch), BF16), vm((1, tile_h, tile_w, ch), F32)),
            in_specs=[pl.BlockSpec(memory_space=pltpu.HBM)] * 6,
            out_specs=(pl.BlockSpec(memory_space=vm),) * 2,
            scratch_shapes=scratch,
            compiler_params=pltpu.CompilerParams(collective_id=0, has_side_effects=True, vmem_limit_bytes=VMEM_LIMIT),
            name="convgru",
        )(*[pltpu.with_memory_space_constraint(v, pltpu.HBM) for v in (jnp.swapaxes(frames, 3, 4), h_init, w_x, w_hzr, w_hn, gate_bias)])

    return jax.shard_map(local_fn, mesh=mesh, in_specs=(frame_spec, state_spec, P(), P(), P(), P()), out_specs=(frame_spec, state_spec), check_vma=False)
```

```python
import jax
import jax.numpy as jnp
from jax import lax
from jax.experimental import pallas as pl
from jax.experimental.pallas import tpu as pltpu
from jax.sharding import PartitionSpec as P

BF16 = jnp.bfloat16
F32 = jnp.float32
MESH = pl.DeviceIdType.MESH
LANES = 128
COL_HALO = 8
CHUNKS = (6,) * 4
UNROLL = 2
AHEAD = 4
PART = 4
VMEM_LIMIT = 40 * 1024 * 1024
NAMES = ("batch", "cols", "rows")


def sigmoid(v):
    return 0.5 * jnp.tanh(0.5 * v) + 0.5


def kernel_body(n_cols, n_rows, dims, frames, h_init, w_x, w_hzr, w_hn, bias, h_seq, h_last,
                wzr, wn, wx, bv, fv, fp, fcs, fcr, fkr, hb, rb, xp, xe, af, hraw, h32, zb, hf, hl, cs, cr, kr, cb,
                load_sem, fsend, frecv, csend, crecv, ksend, krecv, vsend, vrecv):
    steps, tile_h, tile_w, cin, ch = dims
    edge_cells = ((0, 0, 0), (0, 1, 1), (1, 0, tile_w - 2), (1, 1, tile_w - 1))
    batch = lax.axis_index("batch")
    col = lax.axis_index("cols")
    row = lax.axis_index("rows")
    flip = lax.rem(row, 2)
    first_row = row - 1 + 2 * flip
    last_row = row + 1 - 2 * flip
    has_first = jnp.logical_and(first_row >= 0, first_row < n_rows)
    has_last = jnp.logical_and(last_row >= 0, last_row < n_rows)
    has_left = col > 0
    has_right = col < n_cols - 1
    both = jnp.logical_and
    left_dev = (batch, col - 1, row)
    right_dev = (batch, col + 1, row)
    first_dev = (batch, col, first_row)
    last_dev = (batch, col, last_row)
    corner_ok = (both(has_first, has_left), both(has_first, has_right), both(has_last, has_left), both(has_last, has_right))
    corner_dev = ((batch, col - 1, first_row), (batch, col + 1, first_row), (batch, col - 1, last_row), (batch, col + 1, last_row))
    around = ((has_left, left_dev), (has_right, right_dev), (has_first, first_dev), (has_last, last_dev)) + tuple(zip(corner_ok, corner_dev))

    def phys(i):
        return i + flip * (tile_h - 1 - 2 * i)

    n_chunks = len(CHUNKS)
    starts = [sum(CHUNKS[:k]) for k in range(n_chunks)]
    n_ranges = [(starts[k], CHUNKS[k]) for k in range(n_chunks)]
    r_ranges = []
    for k in range(n_chunks):
        lo = -1 if k == 0 else starts[k] + 1
        hi = tile_h + 1 if k == n_chunks - 1 else starts[k] + CHUNKS[k] + 1
        r_ranges.append((lo, hi - lo))

    sides = ((has_left, left_dev), (has_right, right_dev))

    def remote(src, dst, s_sem, r_sem, dev):
        return pltpu.make_async_remote_copy(src_ref=src, dst_ref=dst, send_sem=s_sem, recv_sem=r_sem, device_id=dev, device_id_type=MESH)

    def chunk_rows(k):
        i0, n = n_ranges[k]
        return pl.ds(i0 + flip * (tile_h - n - 2 * i0), n)

    loads = [pltpu.make_async_copy(h_init.at[0, chunk_rows(k)], hraw.at[chunk_rows(k)], load_sem.at[0, k]) for k in range(n_chunks)]
    frame_loads = [pltpu.make_async_copy(frames.at[:, 0], fv, load_sem.at[1, 0])]
    weight_loads = []
    for a in range(3):
        la = a + flip * (2 - 2 * a)
        weight_loads.append(pltpu.make_async_copy(w_hzr.at[a], wzr.at[la], load_sem.at[2, a]))
        weight_loads.append(pltpu.make_async_copy(w_hn.at[a], wn.at[la], load_sem.at[2, 3 + a]))
        for c in range(3):
            dst = wx.at[pl.ds(pl.multiple_of(64 * c + cin * la, cin), cin)]
            weight_loads.append(pltpu.make_async_copy(w_x.at[a, c], dst, load_sem.at[2, 6 + 3 * a + c]))
    weight_loads.append(pltpu.make_async_copy(bias, bv, load_sem.at[2, 15]))
    for copy in frame_loads + loads + weight_loads:
        copy.start()

    hf[...] = jnp.zeros_like(hf)
    hl[...] = jnp.zeros_like(hl)
    cr[...] = jnp.zeros_like(cr)
    kr[...] = jnp.zeros_like(kr)
    cb[...] = jnp.zeros_like(cb)
    fcr[...] = jnp.zeros_like(fcr)
    fkr[...] = jnp.zeros_like(fkr)
    for i in (0, 1, tile_h + 2, tile_h + 3):
        fp[i] = jnp.zeros_like(fp[i])
    for lo in (0, COL_HALO + tile_w):
        fp[:, lo:lo + COL_HALO, :] = jnp.zeros((tile_h + 4, COL_HALO, LANES), F32)
    for lo, hi in ((48, 64), (112, 128), (176, 256)):
        wx[lo:hi] = jnp.zeros((hi - lo, 3 * ch), BF16)

    barrier = pltpu.get_barrier_semaphore()
    count = 0
    for ok, dev in around:
        count = count + ok.astype(jnp.int32)

        @pl.when(ok)
        def _(dev=dev):
            pl.semaphore_signal(barrier, inc=1, device_id=dev, device_id_type=MESH)
    lane = lax.broadcasted_iota(jnp.int32, (1, LANES), 1)

    own_c = pl.ds(COL_HALO, tile_w)

    def pack_frames():
        for i in range(tile_h):
            v = fv[:, phys(i)].reshape(steps * cin, tile_w).astype(F32).T
            fp[i + 2, own_c] = v
            for side, m, x in edge_cells:
                fcs[side, m, pl.ds(i, 1), :] = v[x:x + 1]

    def frame_copies():
        out = [(has_left, remote(fcs.at[0], fcr.at[1], fsend.at[0], frecv.at[1], left_dev), fcr.at[0], frecv.at[0]),
               (has_right, remote(fcs.at[1], fcr.at[0], fsend.at[1], frecv.at[0], right_dev), fcr.at[1], frecv.at[1])]
        rows = ((has_first, first_dev, 2, 1), (has_first, first_dev, 3, 0), (has_last, last_dev, tile_h + 1, tile_h + 2), (has_last, last_dev, tile_h, tile_h + 3))
        for m, (ok, dev, src, dst) in enumerate(rows):
            out.append((ok, remote(fp.at[src, own_c], fp.at[dst, own_c], fsend.at[2 + m], frecv.at[2 + m], dev), fp.at[dst, own_c], frecv.at[2 + m]))
        for q in range(4):
            near = pl.ds(0 if q < 2 else tile_h - 8, 8)
            other = q ^ 1
            out.append((corner_ok[q], remote(fcs.at[q % 2, :, near], fkr.at[other], fsend.at[6 + q], frecv.at[6 + other], corner_dev[q]), fkr.at[q], frecv.at[6 + q]))
        return out

    def place_frames():
        for i in range(tile_h):
            for side, base in ((0, COL_HALO - 2), (1, COL_HALO + tile_w)):
                for m in range(2):
                    fp[i + 2, pl.ds(base + m, 1), :] = fcr[side, m, i:i + 1, :]
        for q in range(4):
            base = COL_HALO - 2 if q % 2 == 0 else COL_HALO + tile_w
            for depth in range(2):
                i = -1 - depth if q < 2 else tile_h + depth
                j = depth if q < 2 else 7 - depth
                for m in range(2):
                    fp[i + 2, pl.ds(base + m, 1), :] = fkr[q, m, j:j + 1, :]

    def chunk_parts(k):
        return range(pl.cdiv(CHUNKS[k], PART))

    def chunk_sends(k, slot):
        out = []
        for p in chunk_parts(k):
            for m, (ok, dev) in enumerate(sides):
                out.append((ok, remote(cs.at[slot, m, k, p], cr.at[slot, 1 - m, k, p], csend.at[slot, m], crecv.at[slot, 1 - m, k, p], dev)))
        return out

    def corner_sends(k, slot):
        out = []
        for edge, q, p in ((0, 0, 0), (n_chunks - 1, 2, (CHUNKS[-1] - 1) // PART)):
            for m in range(2):
                if k == edge:
                    to = q + 1 - m
                    out.append((corner_ok[q + m], remote(cs.at[slot, m, k, p], kr.at[slot, to], ksend.at[slot, q + m], krecv.at[slot, to], corner_dev[q + m])))
        return out

    def row_send(k, slot):
        if k == 0:
            return has_first, remote(h32.at[pl.ds(0, 2)], hf.at[slot], vsend.at[0], vrecv.at[slot, 0], first_dev)
        return has_last, remote(h32.at[pl.ds(tile_h - 2, 2)], hl.at[slot], vsend.at[1], vrecv.at[slot, 1], last_dev)

    def start_sends(k, slot, more):
        copies = chunk_sends(k, slot) + corner_sends(k, slot)
        if k in (0, n_chunks - 1):
            copies.append(row_send(k, slot))
        for ok, copy in copies:
            @pl.when(both(ok, more))
            def _(copy=copy):
                copy.start()

    def wait_chunk_sends(slot, cond):
        copies = [(ok, remote(cs.at[slot, m], cr.at[slot, m], csend.at[slot, m], csend.at[slot, m], dev))
                  for m, (ok, dev) in enumerate(sides)]
        copies += corner_sends(0, slot) + corner_sends(n_chunks - 1, slot)
        for ok, copy in copies:
            @pl.when(both(ok, cond))
            def _(copy=copy):
                copy.wait_send()

    def wait_row_send(k, slot):
        ok, copy = row_send(k, slot)

        @pl.when(ok)
        def _():
            copy.wait_send()

    def wait_if(ok, dst, sem, src):
        @pl.when(ok)
        def _():
            remote(src, dst, csend.at[0, 0], sem, right_dev).wait_recv()

    sub48 = lax.broadcasted_iota(jnp.int32, (tile_w, ch), 0)
    sub16 = lax.broadcasted_iota(jnp.int32, (16, ch), 0)

    def row_of(colbuf, i):
        return cb[colbuf, pl.ds(i + 8, 1), :]

    def publish(slot, i, v, k):
        hb[slot, 1, i + 2] = v.astype(BF16)
        hb[slot, 0, i + 2] = pltpu.roll(v, 1, 0).astype(BF16)
        hb[slot, 2, i + 2] = pltpu.roll(v, tile_w - 1, 0).astype(BF16)
        j = i - starts[k]
        for side, m, x in edge_cells:
            cs[slot, side, k, j // PART, pl.ds(PART * m + j % PART, 1), :] = v[x:x + 1]
        cb[2, pl.ds(i + 8, 1), :] = v[0:1]
        cb[3, pl.ds(i + 8, 1), :] = v[tile_w - 1:tile_w]

    def wait_cols(slot, k, p):
        for m, (ok, _) in enumerate(sides):
            wait_if(ok, cr.at[slot, m, k, p], crecv.at[slot, m, k, p], cs.at[slot, 0, k, p])

    def place_cols(slot, k, p):
        i0, n = n_ranges[k]
        n = min(n - p * PART, PART)
        i0 = i0 + p * PART
        for side in range(2):
            for m in range(2):
                cb[4 * side + m, pl.ds(i0 + 8, n), :] = cr[slot, side, k, p, PART * m:PART * m + n, :]
        for i in range(i0, i0 + n):
            old = hb[slot, 0, i + 2, 0:16].astype(F32)
            hb[slot, 0, i + 2, 0:16] = jnp.where(sub16 == 0, row_of(1, i), old).astype(BF16)
            old = hb[slot, 2, i + 2, tile_w - 16:tile_w].astype(F32)
            hb[slot, 2, i + 2, tile_w - 16:tile_w] = jnp.where(sub16 == 15, row_of(4, i), old).astype(BF16)

    def wait_rows(slot, last):
        src, ok = (hl, has_last) if last else (hf, has_first)
        wait_if(ok, src.at[slot], vrecv.at[slot, last], h32.at[pl.ds(0, 2)])
        for m in range(2):
            q = 2 * last + m
            wait_if(corner_ok[q], kr.at[slot, q], krecv.at[slot, q], cs.at[slot, 0, 0, 0])

    def place_rows(slot, last):
        src = hl if last else hf
        for depth in range(2):
            i = tile_h + depth if last else -1 - depth
            m = 1 - depth if last else depth
            j = (CHUNKS[-1] - 1 - depth if last else depth) % PART
            for x in range(2):
                cb[x, pl.ds(i + 8, 1), :] = kr[slot, 2 * last, PART * x + j:PART * x + j + 1, :]
                cb[4 + x, pl.ds(i + 8, 1), :] = kr[slot, 2 * last + 1, PART * x + j:PART * x + j + 1, :]
            v = src[slot, m]
            cb[2, pl.ds(i + 8, 1), :] = v[0:1]
            cb[3, pl.ds(i + 8, 1), :] = v[tile_w - 1:tile_w]
            hb[slot, 1, i + 2] = v.astype(BF16)
            hb[slot, 0, i + 2] = jnp.where(sub48 == 0, row_of(1, i), pltpu.roll(v, 1, 0)).astype(BF16)
            hb[slot, 2, i + 2] = jnp.where(sub48 == tile_w - 1, row_of(4, i), pltpu.roll(v, tile_w - 1, 0)).astype(BF16)

    wide = tile_w + 2 * COL_HALO

    def build_x(t, k):
        i0, n = r_ranges[k]
        for j in range(n):
            parts = [pltpu.roll(fp[i0 + j + a + 1], lax.rem(cin * a - cin * t + cin * steps, cin * steps), 1) for a in range(3)]
            af[pl.ds(j * wide, wide)] = jnp.where(lane < cin, parts[0], jnp.where(lane < 2 * cin, parts[1], parts[2]))
        for j in range(n):
            base = j * wide + COL_HALO
            left = af[pl.ds(base - 1, tile_w)]
            mid = pltpu.roll(af[pl.ds(base, tile_w)], 64, 1)
            xp[i0 + j + 1, :, 0:LANES] = jnp.where(lane < 64, left, mid).astype(BF16)
            xp[i0 + j + 1, :, LANES:2 * LANES] = af[pl.ds(base + 1, tile_w)].astype(BF16)
        lo_half, hi_half = [], []
        for x in (-1, tile_w):
            three = [af[pl.ds(COL_HALO + x + c - 1, 8, wide)] for c in range(3)]
            lo_half.append(jnp.where(lane < 64, three[0], pltpu.roll(three[1], 64, 1)))
            hi_half.append(three[2])
        xe[k, :, 0:LANES] = jnp.concatenate(lo_half, axis=0).astype(BF16)
        xe[k, :, LANES:2 * LANES] = jnp.concatenate(hi_half, axis=0).astype(BF16)

    all_taps = ["x"] + [(a, c) for c in (1, 0, 2) for a in range(3)]

    def conv(src, i0, n, off, weights, gate, extra=None, e_lo=0, taps=all_taps, acc=None):
        lo, w_lo = gate * ch, (0 if gate == 2 else gate * ch)
        for tap in taps:
            if tap == "x":
                lhs = xp[pl.ds(i0 + 1, n)].reshape(n * tile_w, ch)
                more = None if extra is None else xe[extra]
                weight = wx[:, lo:lo + ch]
            else:
                a, c = tap
                lhs = src(c, pl.ds(i0 + a - 1 - off, n)).reshape(n * tile_w, ch)
                more = None if extra is None else jnp.concatenate(
                    [cb[3 * side + c, pl.ds(e_lo + a - 1 + 8, 8), :] for side in range(2)], axis=0).astype(BF16)
                weight = weights[a, c, :, w_lo:w_lo + ch]
            if more is not None:
                lhs = jnp.concatenate([lhs, more], axis=0)
            part = jnp.dot(lhs, weight, preferred_element_type=F32)
            acc = part if acc is None else acc + part
        return acc

    def biased(acc, gate):
        return acc + bv[gate * ch:(gate + 1) * ch].reshape(1, ch)

    for copy in frame_loads:
        copy.wait()
    pack_frames()
    f_descs = frame_copies()
    pl.semaphore_wait(barrier, count)
    for ok, copy, _, _ in f_descs:
        @pl.when(ok)
        def _(copy=copy):
            copy.start()
    for k in range(n_chunks):
        loads[k].wait()
    for k in range(n_chunks):
        i0, n = n_ranges[k]
        for i in range(i0, i0 + n):
            v = hraw[phys(i)]
            h32[i] = v
            publish(0, i, v, k)
    for k in range(n_chunks):
        start_sends(k, 0, True)
    for ok, copy, _, _ in f_descs:
        @pl.when(ok)
        def _(copy=copy):
            copy.wait_send()
    for copy in weight_loads:
        copy.wait()
    for ok, copy, dst, sem in f_descs:
        @pl.when(ok)
        def _(dst=dst, sem=sem):
            remote(dst, dst, fsend.at[0], sem, right_dev).wait_recv()
    place_frames()
    build_x(0, 0)

    def halves(i0, n):
        return (i0, n - n // 2), (i0 + n - n // 2, n // 2)

    def meet(t, now, k):
        new = 1 - now
        if k == 0:
            start_sends(n_chunks - 1, now, both(t > 0, True))
            free_slot(t, now)
            wait_rows(now, 0)
            wait_row_send(0, now)
        else:
            start_sends(k - 1, new, t < steps - 1)
        fresh = [(k, p) for p in chunk_parts(k) if p or not k]
        if k + 1 < n_chunks:
            fresh.append((k + 1, 0))
        else:
            wait_rows(now, 1)
            wait_row_send(n_chunks - 1, now)
        for item in fresh:
            wait_cols(now, *item)
        for item in fresh:
            place_cols(now, *item)
        if k == 0:
            place_rows(now, 0)
        if k + 1 == n_chunks:
            place_rows(now, 1)

    def free_slot(t, now):
        new = 1 - now
        wait_chunk_sends(new, t >= 1)

    def ahead(now, k):
        out = []
        for h, (i0, n) in enumerate(halves(*n_ranges[k])):
            skip = 0 if k == 0 and h == 0 else 2 if k == n_chunks - 1 and h == 1 else None
            taps = [tap for tap in all_taps[:AHEAD] if tap == "x" or tap[0] != skip]
            acc = conv(lambda c, rows: hb[now, c, rows], i0, n, -2, wzr, 0, taps=taps)
            out.append((taps, acc))
        return out

    def stretch(t, now, k, begun, carry_on):
        new = 1 - now
        meet(t, now, k)
        r_lo, r_n = r_ranges[k]
        parts = halves(r_lo, r_n)
        accs = [conv(lambda c, rows: hb[now, c, rows], i0, n, -2, wzr, 1, extra=k if h == k % 2 else None, e_lo=r_lo) for h, (i0, n) in enumerate(parts)]
        gates = [sigmoid(biased(acc, 1)) for acc in accs]
        ends = gates[k % 2][parts[k % 2][1] * tile_w:]
        ends_l = ends[0:8] * cb[1, pl.ds(r_lo + 8, 8), :]
        ends_r = ends[8:16] * cb[4, pl.ds(r_lo + 8, 8), :]
        for (i0, n), gate in zip(parts, gates):
            for j in range(n):
                i = i0 + j
                e = i - r_lo
                old = hf[now, 0] if i == -1 else hl[now, 1] if i == tile_h else h32[i]
                v = gate[j * tile_w:(j + 1) * tile_w] * old
                rb[1, i + 1] = v.astype(BF16)
                rb[0, i + 1] = jnp.where(sub48 == 0, ends_l[e:e + 1], pltpu.roll(v, 1, 0)).astype(BF16)
                rb[2, i + 1] = jnp.where(sub48 == tile_w - 1, ends_r[e:e + 1], pltpu.roll(v, tile_w - 1, 0)).astype(BF16)
        parts = halves(*n_ranges[k])
        for h, (i0, n) in enumerate(parts):
            done, acc = begun[h] if begun is not None else ([], None)
            acc = conv(lambda c, rows: hb[now, c, rows], i0, n, -2, wzr, 0, taps=[tap for tap in all_taps if tap not in done], acc=acc)
            zb[pl.ds((i0 - n_ranges[k][0]) * tile_w, n * tile_w)] = sigmoid(biased(acc, 0))
        if k + 1 < n_chunks:
            build_x(t, k + 1)
        else:
            build_x(jnp.minimum(t + 1, steps - 1), 0)
        accs = [conv(lambda c, rows: rb[c, rows], i0, n, -1, wn, 2) for i0, n in parts]
        begun = None
        if carry_on and k + 1 < n_chunks:
            begun = ahead(now, k + 1)
        for (i0, n), acc in zip(parts, accs):
            cand = jnp.tanh(biased(acc, 2))
            for j in range(n):
                i = i0 + j
                mix = cand[j * tile_w:(j + 1) * tile_w]
                v = mix + zb[pl.ds((i - n_ranges[k][0]) * tile_w, tile_w)] * (h32[i] - mix)
                h32[i] = v
                h_seq[t, 0, phys(i)] = v.astype(BF16)
                publish(new, i, v, k)
        if carry_on and k + 1 == n_chunks:
            begun = ahead(new, 0)
        return begun

    def body(p, carry):
        begun = None
        for s in range(UNROLL):
            for k in range(n_chunks):
                last = s == UNROLL - 1 and k == n_chunks - 1
                begun = stretch(UNROLL * p + s, s % 2, k, begun, not last)
        return carry

    lax.fori_loop(0, steps // UNROLL, body, 0)
    wait_chunk_sends((steps - 1) % 2, True)
    for i in range(tile_h):
        h_last[0, phys(i)] = h32[i]


def solution(mesh):
    n_rows, n_cols = mesh.shape["rows"], mesh.shape["cols"]
    frame_spec = P(None, "batch", "rows", "cols", None)
    state_spec = P("batch", "rows", "cols", None)

    def local_fn(frames, h_init, w_x, w_hzr, w_hn, gate_bias):
        steps, _, tile_h, tile_w, cin = frames.shape
        ch = h_init.shape[-1]
        dims = (steps, tile_h, tile_w, cin, ch)
        vm = pltpu.VMEM
        dma = pltpu.SemaphoreType.DMA
        kk = len(CHUNKS)
        wide = tile_w + 2 * COL_HALO
        pair = (2, 2)
        scratch = [
            vm((3, 3, ch, 2 * ch), BF16), vm((3, 3, ch, ch), BF16), vm((256, 3 * ch), BF16), vm((3 * ch,), F32),
            vm((steps, tile_h, cin, tile_w), BF16), vm((tile_h + 4, wide, LANES), F32),
            vm(pair + (tile_h, LANES), F32), vm(pair + (tile_h, LANES), F32), vm((4, 2, 8, LANES), F32),
            vm((2, 3, tile_h + 4, tile_w, ch), BF16), vm((3, tile_h + 2, tile_w, ch), BF16),
            vm((tile_h + 2, tile_w, ch), BF16), vm((kk, 16, ch), BF16), vm((8 * wide, LANES), F32),
            vm((tile_h, tile_w, ch), F32), vm((tile_h, tile_w, ch), F32), vm((max(CHUNKS) * tile_w, ch), F32),
            vm(pair + (tile_w, ch), F32), vm(pair + (tile_w, ch), F32),
            vm(pair + (kk, 2, 8, ch), F32), vm(pair + (kk, 2, 8, ch), F32), vm((2, 4, 8, ch), F32), vm((6, 48, ch), F32),
            dma((3, tile_h)), dma((10,)), dma((10,)), dma(pair), dma(pair + (kk, 2)), dma((2, 4)), dma((2, 4)),
            dma((2,)), dma(pair),
        ]

        def body(*refs):
            kernel_body(n_cols, n_rows, dims, *refs)

        return pl.pallas_call(
            body,
            out_shape=(vm((steps, 1, tile_h, tile_w, ch), BF16), vm((1, tile_h, tile_w, ch), F32)),
            in_specs=[pl.BlockSpec(memory_space=pltpu.HBM)] * 6,
            out_specs=(pl.BlockSpec(memory_space=vm),) * 2,
            scratch_shapes=scratch,
            compiler_params=pltpu.CompilerParams(collective_id=0, has_side_effects=True, vmem_limit_bytes=VMEM_LIMIT),
            name="convgru",
        )(*[pltpu.with_memory_space_constraint(v, pltpu.HBM) for v in (jnp.swapaxes(frames, 3, 4), h_init, w_x, w_hzr, w_hn, gate_bias)])

    return jax.shard_map(local_fn, mesh=mesh, in_specs=(frame_spec, state_spec, P(), P(), P(), P()), out_specs=(frame_spec, state_spec), check_vma=False)
```

```python
import jax
import jax.numpy as jnp
from jax import lax
from jax.experimental import pallas as pl
from jax.experimental.pallas import tpu as pltpu
from jax.sharding import PartitionSpec as P

BF16 = jnp.bfloat16
F32 = jnp.float32
MESH = pl.DeviceIdType.MESH
LANES = 128
COL_HALO = 8
CHUNKS = (6,) * 4
UNROLL = 2
AHEAD = 4
PART = 4
VMEM_LIMIT = 40 * 1024 * 1024
NAMES = ("batch", "cols", "rows")


def sigmoid(v):
    return 0.5 * jnp.tanh(0.5 * v) + 0.5


def kernel_body(n_cols, n_rows, dims, frames, h_init, w_x, w_hzr, w_hn, bias, h_seq, h_last,
                wzr, wn, wx, bv, fv, fp, fcs, fcr, fkr, hb, rb, xp, xe, af, hraw, h32, zb, hf, hl, cs, cr, kr, cb,
                load_sem, fsend, frecv, csend, crecv, ksend, krecv, vsend, vrecv):
    steps, tile_h, tile_w, cin, ch = dims
    edge_cells = ((0, 0, 0), (0, 1, 1), (1, 0, tile_w - 2), (1, 1, tile_w - 1))
    batch = lax.axis_index("batch")
    col = lax.axis_index("cols")
    row = lax.axis_index("rows")
    flip = lax.rem(row, 2)
    first_row = row - 1 + 2 * flip
    last_row = row + 1 - 2 * flip
    has_first = jnp.logical_and(first_row >= 0, first_row < n_rows)
    has_last = jnp.logical_and(last_row >= 0, last_row < n_rows)
    has_left = col > 0
    has_right = col < n_cols - 1
    both = jnp.logical_and
    left_dev = (batch, col - 1, row)
    right_dev = (batch, col + 1, row)
    first_dev = (batch, col, first_row)
    last_dev = (batch, col, last_row)
    corner_ok = (both(has_first, has_left), both(has_first, has_right), both(has_last, has_left), both(has_last, has_right))
    corner_dev = ((batch, col - 1, first_row), (batch, col + 1, first_row), (batch, col - 1, last_row), (batch, col + 1, last_row))
    around = ((has_left, left_dev), (has_right, right_dev), (has_first, first_dev), (has_last, last_dev)) + tuple(zip(corner_ok, corner_dev))

    def phys(i):
        return i + flip * (tile_h - 1 - 2 * i)

    n_chunks = len(CHUNKS)
    starts = [sum(CHUNKS[:k]) for k in range(n_chunks)]
    n_ranges = [(starts[k], CHUNKS[k]) for k in range(n_chunks)]
    r_ranges = []
    for k in range(n_chunks):
        lo = -1 if k == 0 else starts[k] + 1
        hi = tile_h + 1 if k == n_chunks - 1 else starts[k] + CHUNKS[k] + 1
        r_ranges.append((lo, hi - lo))

    sides = ((has_left, left_dev), (has_right, right_dev))

    def remote(src, dst, s_sem, r_sem, dev):
        return pltpu.make_async_remote_copy(src_ref=src, dst_ref=dst, send_sem=s_sem, recv_sem=r_sem, device_id=dev, device_id_type=MESH)

    def chunk_rows(k):
        i0, n = n_ranges[k]
        return pl.ds(i0 + flip * (tile_h - n - 2 * i0), n)

    loads = [pltpu.make_async_copy(h_init.at[0, chunk_rows(k)], hraw.at[chunk_rows(k)], load_sem.at[0, k]) for k in range(n_chunks)]
    frame_loads = [pltpu.make_async_copy(frames.at[:, 0], fv, load_sem.at[1, 0])]
    weight_loads = []
    for a in range(3):
        la = a + flip * (2 - 2 * a)
        weight_loads.append(pltpu.make_async_copy(w_hzr.at[a], wzr.at[la], load_sem.at[2, a]))
        weight_loads.append(pltpu.make_async_copy(w_hn.at[a], wn.at[la], load_sem.at[2, 3 + a]))
        for c in range(3):
            dst = wx.at[pl.ds(pl.multiple_of(64 * c + cin * la, cin), cin)]
            weight_loads.append(pltpu.make_async_copy(w_x.at[a, c], dst, load_sem.at[2, 6 + 3 * a + c]))
    weight_loads.append(pltpu.make_async_copy(bias, bv, load_sem.at[2, 15]))
    for copy in frame_loads + loads + weight_loads:
        copy.start()

    hf[...] = jnp.zeros_like(hf)
    hl[...] = jnp.zeros_like(hl)
    cr[...] = jnp.zeros_like(cr)
    kr[...] = jnp.zeros_like(kr)
    cb[...] = jnp.zeros_like(cb)
    fcr[...] = jnp.zeros_like(fcr)
    fkr[...] = jnp.zeros_like(fkr)
    for i in (0, 1, tile_h + 2, tile_h + 3):
        fp[i] = jnp.zeros_like(fp[i])
    for lo in (0, COL_HALO + tile_w):
        fp[:, lo:lo + COL_HALO, :] = jnp.zeros((tile_h + 4, COL_HALO, LANES), F32)
    for lo, hi in ((48, 64), (112, 128), (176, 256)):
        wx[lo:hi] = jnp.zeros((hi - lo, 3 * ch), BF16)

    barrier = pltpu.get_barrier_semaphore()
    count = 0
    for ok, dev in around:
        count = count + ok.astype(jnp.int32)

        @pl.when(ok)
        def _(dev=dev):
            pl.semaphore_signal(barrier, inc=1, device_id=dev, device_id_type=MESH)
    lane = lax.broadcasted_iota(jnp.int32, (1, LANES), 1)

    own_c = pl.ds(COL_HALO, tile_w)

    def pack_frames():
        for i in range(tile_h):
            v = fv[:, phys(i)].reshape(steps * cin, tile_w).astype(F32).T
            fp[i + 2, own_c] = v
            for side, m, x in edge_cells:
                fcs[side, m, pl.ds(i, 1), :] = v[x:x + 1]

    def frame_copies():
        out = [(has_left, remote(fcs.at[0], fcr.at[1], fsend.at[0], frecv.at[1], left_dev), fcr.at[0], frecv.at[0]),
               (has_right, remote(fcs.at[1], fcr.at[0], fsend.at[1], frecv.at[0], right_dev), fcr.at[1], frecv.at[1])]
        rows = ((has_first, first_dev, 2, 1), (has_first, first_dev, 3, 0), (has_last, last_dev, tile_h + 1, tile_h + 2), (has_last, last_dev, tile_h, tile_h + 3))
        for m, (ok, dev, src, dst) in enumerate(rows):
            out.append((ok, remote(fp.at[src, own_c], fp.at[dst, own_c], fsend.at[2 + m], frecv.at[2 + m], dev), fp.at[dst, own_c], frecv.at[2 + m]))
        for q in range(4):
            near = pl.ds(0 if q < 2 else tile_h - 8, 8)
            other = q ^ 1
            out.append((corner_ok[q], remote(fcs.at[q % 2, :, near], fkr.at[other], fsend.at[6 + q], frecv.at[6 + other], corner_dev[q]), fkr.at[q], frecv.at[6 + q]))
        return out

    def place_frames():
        for i in range(tile_h):
            for side, base in ((0, COL_HALO - 2), (1, COL_HALO + tile_w)):
                for m in range(2):
                    fp[i + 2, pl.ds(base + m, 1), :] = fcr[side, m, i:i + 1, :]
        for q in range(4):
            base = COL_HALO - 2 if q % 2 == 0 else COL_HALO + tile_w
            for depth in range(2):
                i = -1 - depth if q < 2 else tile_h + depth
                j = depth if q < 2 else 7 - depth
                for m in range(2):
                    fp[i + 2, pl.ds(base + m, 1), :] = fkr[q, m, j:j + 1, :]

    def chunk_parts(k):
        return range(pl.cdiv(CHUNKS[k], PART))

    def chunk_sends(k, slot):
        out = []
        for p in chunk_parts(k):
            for m, (ok, dev) in enumerate(sides):
                out.append((ok, remote(cs.at[slot, m, k, p], cr.at[slot, 1 - m, k, p], csend.at[slot, m], crecv.at[slot, 1 - m, k, p], dev)))
        return out

    def corner_sends(k, slot):
        out = []
        for edge, q, p in ((0, 0, 0), (n_chunks - 1, 2, (CHUNKS[-1] - 1) // PART)):
            for m in range(2):
                if k == edge:
                    to = q + 1 - m
                    out.append((corner_ok[q + m], remote(cs.at[slot, m, k, p], kr.at[slot, to], ksend.at[slot, q + m], krecv.at[slot, to], corner_dev[q + m])))
        return out

    def row_send(k, slot):
        if k == 0:
            return has_first, remote(h32.at[pl.ds(0, 2)], hf.at[slot], vsend.at[0], vrecv.at[slot, 0], first_dev)
        return has_last, remote(h32.at[pl.ds(tile_h - 2, 2)], hl.at[slot], vsend.at[1], vrecv.at[slot, 1], last_dev)

    def start_sends(k, slot, more):
        copies = chunk_sends(k, slot) + corner_sends(k, slot)
        if k in (0, n_chunks - 1):
            copies.append(row_send(k, slot))
        for ok, copy in copies:
            @pl.when(both(ok, more))
            def _(copy=copy):
                copy.start()

    def wait_chunk_sends(slot, cond):
        copies = [(ok, remote(cs.at[slot, m], cr.at[slot, m], csend.at[slot, m], csend.at[slot, m], dev))
                  for m, (ok, dev) in enumerate(sides)]
        copies += corner_sends(0, slot) + corner_sends(n_chunks - 1, slot)
        for ok, copy in copies:
            @pl.when(both(ok, cond))
            def _(copy=copy):
                copy.wait_send()

    def wait_row_send(k, slot):
        ok, copy = row_send(k, slot)

        @pl.when(ok)
        def _():
            copy.wait_send()

    def wait_if(ok, dst, sem, src):
        @pl.when(ok)
        def _():
            remote(src, dst, csend.at[0, 0], sem, right_dev).wait_recv()

    sub48 = lax.broadcasted_iota(jnp.int32, (tile_w, ch), 0)
    sub16 = lax.broadcasted_iota(jnp.int32, (16, ch), 0)

    def row_of(colbuf, i):
        return cb[colbuf, pl.ds(i + 8, 1), :]

    def publish(slot, i, v, k):
        hb[slot, 1, i + 2] = v.astype(BF16)
        hb[slot, 0, i + 2] = pltpu.roll(v, 1, 0).astype(BF16)
        hb[slot, 2, i + 2] = pltpu.roll(v, tile_w - 1, 0).astype(BF16)
        j = i - starts[k]
        for side, m, x in edge_cells:
            cs[slot, side, k, j // PART, pl.ds(PART * m + j % PART, 1), :] = v[x:x + 1]
        cb[2, pl.ds(i + 8, 1), :] = v[0:1]
        cb[3, pl.ds(i + 8, 1), :] = v[tile_w - 1:tile_w]

    def wait_cols(slot, k, p):
        for m, (ok, _) in enumerate(sides):
            wait_if(ok, cr.at[slot, m, k, p], crecv.at[slot, m, k, p], cs.at[slot, 0, k, p])

    def place_cols(slot, k, p):
        i0, n = n_ranges[k]
        n = min(n - p * PART, PART)
        i0 = i0 + p * PART
        for side in range(2):
            for m in range(2):
                cb[4 * side + m, pl.ds(i0 + 8, n), :] = cr[slot, side, k, p, PART * m:PART * m + n, :]
        for i in range(i0, i0 + n):
            old = hb[slot, 0, i + 2, 0:16].astype(F32)
            hb[slot, 0, i + 2, 0:16] = jnp.where(sub16 == 0, row_of(1, i), old).astype(BF16)
            old = hb[slot, 2, i + 2, tile_w - 16:tile_w].astype(F32)
            hb[slot, 2, i + 2, tile_w - 16:tile_w] = jnp.where(sub16 == 15, row_of(4, i), old).astype(BF16)

    def wait_rows(slot, last):
        src, ok = (hl, has_last) if last else (hf, has_first)
        wait_if(ok, src.at[slot], vrecv.at[slot, last], h32.at[pl.ds(0, 2)])
        for m in range(2):
            q = 2 * last + m
            wait_if(corner_ok[q], kr.at[slot, q], krecv.at[slot, q], cs.at[slot, 0, 0, 0])

    def place_rows(slot, last):
        src = hl if last else hf
        for depth in range(2):
            i = tile_h + depth if last else -1 - depth
            m = 1 - depth if last else depth
            j = (CHUNKS[-1] - 1 - depth if last else depth) % PART
            for x in range(2):
                cb[x, pl.ds(i + 8, 1), :] = kr[slot, 2 * last, PART * x + j:PART * x + j + 1, :]
                cb[4 + x, pl.ds(i + 8, 1), :] = kr[slot, 2 * last + 1, PART * x + j:PART * x + j + 1, :]
            v = src[slot, m]
            cb[2, pl.ds(i + 8, 1), :] = v[0:1]
            cb[3, pl.ds(i + 8, 1), :] = v[tile_w - 1:tile_w]
            hb[slot, 1, i + 2] = v.astype(BF16)
            hb[slot, 0, i + 2] = jnp.where(sub48 == 0, row_of(1, i), pltpu.roll(v, 1, 0)).astype(BF16)
            hb[slot, 2, i + 2] = jnp.where(sub48 == tile_w - 1, row_of(4, i), pltpu.roll(v, tile_w - 1, 0)).astype(BF16)

    wide = tile_w + 2 * COL_HALO

    def build_x(t, k):
        i0, n = r_ranges[k]
        for j in range(n):
            parts = [pltpu.roll(fp[i0 + j + a + 1], lax.rem(cin * a - cin * t + cin * steps, cin * steps), 1) for a in range(3)]
            af[pl.ds(j * wide, wide)] = jnp.where(lane < cin, parts[0], jnp.where(lane < 2 * cin, parts[1], parts[2]))
        for j in range(n):
            base = j * wide + COL_HALO
            left = af[pl.ds(base - 1, tile_w)]
            mid = pltpu.roll(af[pl.ds(base, tile_w)], 64, 1)
            xp[i0 + j + 1, :, 0:LANES] = jnp.where(lane < 64, left, mid).astype(BF16)
            xp[i0 + j + 1, :, LANES:2 * LANES] = af[pl.ds(base + 1, tile_w)].astype(BF16)
        lo_half, hi_half = [], []
        for x in (-1, tile_w):
            three = [af[pl.ds(COL_HALO + x + c - 1, 8, wide)] for c in range(3)]
            lo_half.append(jnp.where(lane < 64, three[0], pltpu.roll(three[1], 64, 1)))
            hi_half.append(three[2])
        xe[k, :, 0:LANES] = jnp.concatenate(lo_half, axis=0).astype(BF16)
        xe[k, :, LANES:2 * LANES] = jnp.concatenate(hi_half, axis=0).astype(BF16)

    all_taps = ["x"] + [(a, c) for c in (1, 0, 2) for a in range(3)]

    def conv(src, i0, n, off, weights, gate, extra=None, e_lo=0, taps=all_taps, acc=None):
        lo, w_lo = gate * ch, (0 if gate == 2 else gate * ch)
        for tap in taps:
            if tap == "x":
                lhs = xp[pl.ds(i0 + 1, n)].reshape(n * tile_w, ch)
                more = None if extra is None else xe[extra]
                weight = wx[:, lo:lo + ch]
            else:
                a, c = tap
                lhs = src(c, pl.ds(i0 + a - 1 - off, n)).reshape(n * tile_w, ch)
                more = None if extra is None else jnp.concatenate(
                    [cb[3 * side + c, pl.ds(e_lo + a - 1 + 8, 8), :] for side in range(2)], axis=0).astype(BF16)
                weight = weights[a, c, :, w_lo:w_lo + ch]
            if more is not None:
                lhs = jnp.concatenate([lhs, more], axis=0)
            part = jnp.dot(lhs, weight, preferred_element_type=F32)
            acc = part if acc is None else acc + part
        return acc

    def biased(acc, gate):
        return acc + bv[gate * ch:(gate + 1) * ch].reshape(1, ch)

    for copy in frame_loads:
        copy.wait()
    pack_frames()
    f_descs = frame_copies()
    pl.semaphore_wait(barrier, count)
    for ok, copy, _, _ in f_descs:
        @pl.when(ok)
        def _(copy=copy):
            copy.start()
    for group in ((0, 1), range(2, n_chunks)):
        for k in group:
            loads[k].wait()
        for k in group:
            i0, n = n_ranges[k]
            for i in range(i0, i0 + n):
                v = hraw[phys(i)]
                h32[i] = v
                publish(0, i, v, k)
        for k in group:
            start_sends(k, 0, True)
    for ok, copy, _, _ in f_descs:
        @pl.when(ok)
        def _(copy=copy):
            copy.wait_send()
    for copy in weight_loads:
        copy.wait()
    for ok, copy, dst, sem in f_descs:
        @pl.when(ok)
        def _(dst=dst, sem=sem):
            remote(dst, dst, fsend.at[0], sem, right_dev).wait_recv()
    place_frames()
    build_x(0, 0)

    def halves(i0, n):
        return (i0, n - n // 2), (i0 + n - n // 2, n // 2)

    def meet(t, now, k):
        new = 1 - now
        if k == 0:
            start_sends(n_chunks - 1, now, both(t > 0, True))
            free_slot(t, now)
            wait_rows(now, 0)
            wait_row_send(0, now)
        else:
            start_sends(k - 1, new, t < steps - 1)
        fresh = [(k, p) for p in chunk_parts(k) if p or not k]
        if k + 1 < n_chunks:
            fresh.append((k + 1, 0))
        else:
            wait_rows(now, 1)
            wait_row_send(n_chunks - 1, now)
        for item in fresh:
            wait_cols(now, *item)
        for item in fresh:
            place_cols(now, *item)
        if k == 0:
            place_rows(now, 0)
        if k + 1 == n_chunks:
            place_rows(now, 1)

    def free_slot(t, now):
        new = 1 - now
        wait_chunk_sends(new, t >= 1)

    def ahead(now, k):
        out = []
        for h, (i0, n) in enumerate(halves(*n_ranges[k])):
            skip = 0 if k == 0 and h == 0 else 2 if k == n_chunks - 1 and h == 1 else None
            taps = [tap for tap in all_taps[:AHEAD] if tap == "x" or tap[0] != skip]
            acc = conv(lambda c, rows: hb[now, c, rows], i0, n, -2, wzr, 0, taps=taps)
            out.append((taps, acc))
        return out

    def stretch(t, now, k, begun, carry_on):
        new = 1 - now
        meet(t, now, k)
        r_lo, r_n = r_ranges[k]
        parts = halves(r_lo, r_n)
        accs = [conv(lambda c, rows: hb[now, c, rows], i0, n, -2, wzr, 1, extra=k if h == k % 2 else None, e_lo=r_lo) for h, (i0, n) in enumerate(parts)]
        gates = [sigmoid(biased(acc, 1)) for acc in accs]
        ends = gates[k % 2][parts[k % 2][1] * tile_w:]
        ends_l = ends[0:8] * cb[1, pl.ds(r_lo + 8, 8), :]
        ends_r = ends[8:16] * cb[4, pl.ds(r_lo + 8, 8), :]
        for (i0, n), gate in zip(parts, gates):
            for j in range(n):
                i = i0 + j
                e = i - r_lo
                old = hf[now, 0] if i == -1 else hl[now, 1] if i == tile_h else h32[i]
                v = gate[j * tile_w:(j + 1) * tile_w] * old
                rb[1, i + 1] = v.astype(BF16)
                rb[0, i + 1] = jnp.where(sub48 == 0, ends_l[e:e + 1], pltpu.roll(v, 1, 0)).astype(BF16)
                rb[2, i + 1] = jnp.where(sub48 == tile_w - 1, ends_r[e:e + 1], pltpu.roll(v, tile_w - 1, 0)).astype(BF16)
        parts = halves(*n_ranges[k])
        for h, (i0, n) in enumerate(parts):
            done, acc = begun[h] if begun is not None else ([], None)
            acc = conv(lambda c, rows: hb[now, c, rows], i0, n, -2, wzr, 0, taps=[tap for tap in all_taps if tap not in done], acc=acc)
            zb[pl.ds((i0 - n_ranges[k][0]) * tile_w, n * tile_w)] = sigmoid(biased(acc, 0))
        if k + 1 < n_chunks:
            build_x(t, k + 1)
        else:
            build_x(jnp.minimum(t + 1, steps - 1), 0)
        accs = [conv(lambda c, rows: rb[c, rows], i0, n, -1, wn, 2) for i0, n in parts]
        begun = None
        if carry_on and k + 1 < n_chunks:
            begun = ahead(now, k + 1)
        for (i0, n), acc in zip(parts, accs):
            cand = jnp.tanh(biased(acc, 2))
            for j in range(n):
                i = i0 + j
                mix = cand[j * tile_w:(j + 1) * tile_w]
                v = mix + zb[pl.ds((i - n_ranges[k][0]) * tile_w, tile_w)] * (h32[i] - mix)
                h32[i] = v
                h_seq[t, 0, phys(i)] = v.astype(BF16)
                publish(new, i, v, k)
        if carry_on and k + 1 == n_chunks:
            begun = ahead(new, 0)
        return begun

    def body(p, carry):
        begun = None
        for s in range(UNROLL):
            for k in range(n_chunks):
                last = s == UNROLL - 1 and k == n_chunks - 1
                begun = stretch(UNROLL * p + s, s % 2, k, begun, not last)
        return carry

    lax.fori_loop(0, steps // UNROLL, body, 0)
    wait_chunk_sends((steps - 1) % 2, True)
    for i in range(tile_h):
        h_last[0, phys(i)] = h32[i]


def solution(mesh):
    n_rows, n_cols = mesh.shape["rows"], mesh.shape["cols"]
    frame_spec = P(None, "batch", "rows", "cols", None)
    state_spec = P("batch", "rows", "cols", None)

    def local_fn(frames, h_init, w_x, w_hzr, w_hn, gate_bias):
        steps, _, tile_h, tile_w, cin = frames.shape
        ch = h_init.shape[-1]
        dims = (steps, tile_h, tile_w, cin, ch)
        vm = pltpu.VMEM
        dma = pltpu.SemaphoreType.DMA
        kk = len(CHUNKS)
        wide = tile_w + 2 * COL_HALO
        pair = (2, 2)
        scratch = [
            vm((3, 3, ch, 2 * ch), BF16), vm((3, 3, ch, ch), BF16), vm((256, 3 * ch), BF16), vm((3 * ch,), F32),
            vm((steps, tile_h, cin, tile_w), BF16), vm((tile_h + 4, wide, LANES), F32),
            vm(pair + (tile_h, LANES), F32), vm(pair + (tile_h, LANES), F32), vm((4, 2, 8, LANES), F32),
            vm((2, 3, tile_h + 4, tile_w, ch), BF16), vm((3, tile_h + 2, tile_w, ch), BF16),
            vm((tile_h + 2, tile_w, ch), BF16), vm((kk, 16, ch), BF16), vm((8 * wide, LANES), F32),
            vm((tile_h, tile_w, ch), F32), vm((tile_h, tile_w, ch), F32), vm((max(CHUNKS) * tile_w, ch), F32),
            vm(pair + (tile_w, ch), F32), vm(pair + (tile_w, ch), F32),
            vm(pair + (kk, 2, 8, ch), F32), vm(pair + (kk, 2, 8, ch), F32), vm((2, 4, 8, ch), F32), vm((6, 48, ch), F32),
            dma((3, tile_h)), dma((10,)), dma((10,)), dma(pair), dma(pair + (kk, 2)), dma((2, 4)), dma((2, 4)),
            dma((2,)), dma(pair),
        ]

        def body(*refs):
            kernel_body(n_cols, n_rows, dims, *refs)

        results = pl.pallas_call(
            body,
            out_shape=(vm((steps, 1, tile_h, tile_w, ch), BF16), vm((1, tile_h, tile_w, ch), F32)),
            in_specs=[pl.BlockSpec(memory_space=pltpu.HBM)] * 6,
            out_specs=(pl.BlockSpec(memory_space=vm),) * 2,
            scratch_shapes=scratch,
            compiler_params=pltpu.CompilerParams(collective_id=0, has_side_effects=True, vmem_limit_bytes=VMEM_LIMIT),
            name="convgru",
        )(*[pltpu.with_memory_space_constraint(v, pltpu.HBM) for v in (jnp.swapaxes(frames, 3, 4), h_init, w_x, w_hzr, w_hn, gate_bias)])

        def drain(seq_in, last_in, seq_out, last_out, sems):
            copies = [pltpu.make_async_copy(src, dst, sems.at[m]) for m, (src, dst) in enumerate(((seq_in, seq_out), (last_in, last_out)))]
            for copy in copies:
                copy.start()
            for copy in copies:
                copy.wait()

        return pl.pallas_call(
            drain,
            out_shape=[jax.ShapeDtypeStruct(v.shape, v.dtype) for v in results],
            in_specs=[pl.BlockSpec(memory_space=vm)] * 2,
            out_specs=[pl.BlockSpec(memory_space=pltpu.HBM)] * 2,
            scratch_shapes=[dma((2,))],
            compiler_params=pltpu.CompilerParams(vmem_limit_bytes=VMEM_LIMIT // 8),
            name="drain",
        )(*[pltpu.with_memory_space_constraint(v, vm) for v in results])

    return jax.shard_map(local_fn, mesh=mesh, in_specs=(frame_spec, state_spec, P(), P(), P(), P()), out_specs=(frame_spec, state_spec), check_vma=False)
```

```python
import jax
import jax.numpy as jnp
from jax import lax
from jax.experimental import pallas as pl
from jax.experimental.pallas import tpu as pltpu
from jax.sharding import PartitionSpec as P

BF16 = jnp.bfloat16
F32 = jnp.float32
MESH = pl.DeviceIdType.MESH
LANES = 128
COL_HALO = 8
CHUNKS = (6,) * 4
UNROLL = 2
AHEAD = 4
PART = 2
VMEM_LIMIT = 40 * 1024 * 1024
NAMES = ("batch", "cols", "rows")


def sigmoid(v):
    return 0.5 * jnp.tanh(0.5 * v) + 0.5


def kernel_body(n_cols, n_rows, dims, frames, h_init, w_x, w_hzr, w_hn, bias, h_seq, h_last,
                wzr, wn, wx, bv, fv, fp, fcs, fcr, fkr, hb, rb, xp, xe, af, hraw, h32, zb, hf, hl, cs, cr, kr, cb,
                load_sem, fsend, frecv, csend, crecv, ksend, krecv, vsend, vrecv):
    steps, tile_h, tile_w, cin, ch = dims
    edge_cells = ((0, 0, 0), (0, 1, 1), (1, 0, tile_w - 2), (1, 1, tile_w - 1))
    batch = lax.axis_index("batch")
    col = lax.axis_index("cols")
    row = lax.axis_index("rows")
    flip = lax.rem(row, 2)
    first_row = row - 1 + 2 * flip
    last_row = row + 1 - 2 * flip
    has_first = jnp.logical_and(first_row >= 0, first_row < n_rows)
    has_last = jnp.logical_and(last_row >= 0, last_row < n_rows)
    has_left = col > 0
    has_right = col < n_cols - 1
    both = jnp.logical_and
    left_dev = (batch, col - 1, row)
    right_dev = (batch, col + 1, row)
    first_dev = (batch, col, first_row)
    last_dev = (batch, col, last_row)
    corner_ok = (both(has_first, has_left), both(has_first, has_right), both(has_last, has_left), both(has_last, has_right))
    corner_dev = ((batch, col - 1, first_row), (batch, col + 1, first_row), (batch, col - 1, last_row), (batch, col + 1, last_row))
    around = ((has_left, left_dev), (has_right, right_dev), (has_first, first_dev), (has_last, last_dev)) + tuple(zip(corner_ok, corner_dev))

    def phys(i):
        return i + flip * (tile_h - 1 - 2 * i)

    n_chunks = len(CHUNKS)
    starts = [sum(CHUNKS[:k]) for k in range(n_chunks)]
    n_ranges = [(starts[k], CHUNKS[k]) for k in range(n_chunks)]
    r_ranges = []
    for k in range(n_chunks):
        lo = -1 if k == 0 else starts[k] + 1
        hi = tile_h + 1 if k == n_chunks - 1 else starts[k] + CHUNKS[k] + 1
        r_ranges.append((lo, hi - lo))

    sides = ((has_left, left_dev), (has_right, right_dev))

    def remote(src, dst, s_sem, r_sem, dev):
        return pltpu.make_async_remote_copy(src_ref=src, dst_ref=dst, send_sem=s_sem, recv_sem=r_sem, device_id=dev, device_id_type=MESH)

    def chunk_rows(k):
        i0, n = n_ranges[k]
        return pl.ds(i0 + flip * (tile_h - n - 2 * i0), n)

    loads = [pltpu.make_async_copy(h_init.at[0, chunk_rows(k)], hraw.at[chunk_rows(k)], load_sem.at[0, k]) for k in range(n_chunks)]
    frame_loads = [pltpu.make_async_copy(frames.at[:, 0], fv, load_sem.at[1, 0])]
    weight_loads = []
    for a in range(3):
        la = a + flip * (2 - 2 * a)
        weight_loads.append(pltpu.make_async_copy(w_hzr.at[a], wzr.at[la], load_sem.at[2, a]))
        weight_loads.append(pltpu.make_async_copy(w_hn.at[a], wn.at[la], load_sem.at[2, 3 + a]))
        for c in range(3):
            dst = wx.at[pl.ds(pl.multiple_of(64 * c + cin * la, cin), cin)]
            weight_loads.append(pltpu.make_async_copy(w_x.at[a, c], dst, load_sem.at[2, 6 + 3 * a + c]))
    weight_loads.append(pltpu.make_async_copy(bias, bv, load_sem.at[2, 15]))
    for copy in frame_loads + loads + weight_loads:
        copy.start()

    hf[...] = jnp.zeros_like(hf)
    hl[...] = jnp.zeros_like(hl)
    cr[...] = jnp.zeros_like(cr)
    kr[...] = jnp.zeros_like(kr)
    cb[...] = jnp.zeros_like(cb)
    fcr[...] = jnp.zeros_like(fcr)
    fkr[...] = jnp.zeros_like(fkr)
    for i in (0, 1, tile_h + 2, tile_h + 3):
        fp[i] = jnp.zeros_like(fp[i])
    for lo in (0, COL_HALO + tile_w):
        fp[:, lo:lo + COL_HALO, :] = jnp.zeros((tile_h + 4, COL_HALO, LANES), F32)
    for lo, hi in ((48, 64), (112, 128), (176, 256)):
        wx[lo:hi] = jnp.zeros((hi - lo, 3 * ch), BF16)

    barrier = pltpu.get_barrier_semaphore()
    count = 0
    for ok, dev in around:
        count = count + ok.astype(jnp.int32)

        @pl.when(ok)
        def _(dev=dev):
            pl.semaphore_signal(barrier, inc=1, device_id=dev, device_id_type=MESH)
    lane = lax.broadcasted_iota(jnp.int32, (1, LANES), 1)

    own_c = pl.ds(COL_HALO, tile_w)

    def pack_frames():
        for i in range(tile_h):
            v = fv[:, phys(i)].reshape(steps * cin, tile_w).astype(F32).T
            fp[i + 2, own_c] = v
            for side, m, x in edge_cells:
                fcs[side, m, pl.ds(i, 1), :] = v[x:x + 1]

    def frame_copies():
        out = [(has_left, remote(fcs.at[0], fcr.at[1], fsend.at[0], frecv.at[1], left_dev), fcr.at[0], frecv.at[0]),
               (has_right, remote(fcs.at[1], fcr.at[0], fsend.at[1], frecv.at[0], right_dev), fcr.at[1], frecv.at[1])]
        rows = ((has_first, first_dev, 2, 1), (has_first, first_dev, 3, 0), (has_last, last_dev, tile_h + 1, tile_h + 2), (has_last, last_dev, tile_h, tile_h + 3))
        for m, (ok, dev, src, dst) in enumerate(rows):
            out.append((ok, remote(fp.at[src, own_c], fp.at[dst, own_c], fsend.at[2 + m], frecv.at[2 + m], dev), fp.at[dst, own_c], frecv.at[2 + m]))
        for q in range(4):
            near = pl.ds(0 if q < 2 else tile_h - 8, 8)
            other = q ^ 1
            out.append((corner_ok[q], remote(fcs.at[q % 2, :, near], fkr.at[other], fsend.at[6 + q], frecv.at[6 + other], corner_dev[q]), fkr.at[q], frecv.at[6 + q]))
        return out

    def place_frames():
        for i in range(tile_h):
            for side, base in ((0, COL_HALO - 2), (1, COL_HALO + tile_w)):
                for m in range(2):
                    fp[i + 2, pl.ds(base + m, 1), :] = fcr[side, m, i:i + 1, :]
        for q in range(4):
            base = COL_HALO - 2 if q % 2 == 0 else COL_HALO + tile_w
            for depth in range(2):
                i = -1 - depth if q < 2 else tile_h + depth
                j = depth if q < 2 else 7 - depth
                for m in range(2):
                    fp[i + 2, pl.ds(base + m, 1), :] = fkr[q, m, j:j + 1, :]

    def chunk_parts(k):
        return range(pl.cdiv(CHUNKS[k], PART))

    def chunk_sends(k, slot):
        out = []
        for p in chunk_parts(k):
            for m, (ok, dev) in enumerate(sides):
                out.append((ok, remote(cs.at[slot, m, k, p], cr.at[slot, 1 - m, k, p], csend.at[slot, m], crecv.at[slot, 1 - m, k, p], dev)))
        return out

    def corner_sends(k, slot):
        out = []
        for edge, q, p in ((0, 0, 0), (n_chunks - 1, 2, (CHUNKS[-1] - 1) // PART)):
            for m in range(2):
                if k == edge:
                    to = q + 1 - m
                    out.append((corner_ok[q + m], remote(cs.at[slot, m, k, p], kr.at[slot, to], ksend.at[slot, q + m], krecv.at[slot, to], corner_dev[q + m])))
        return out

    def row_send(k, slot):
        if k == 0:
            return has_first, remote(h32.at[pl.ds(0, 2)], hf.at[slot], vsend.at[0], vrecv.at[slot, 0], first_dev)
        return has_last, remote(h32.at[pl.ds(tile_h - 2, 2)], hl.at[slot], vsend.at[1], vrecv.at[slot, 1], last_dev)

    def start_sends(k, slot, more):
        copies = chunk_sends(k, slot) + corner_sends(k, slot)
        if k in (0, n_chunks - 1):
            copies.append(row_send(k, slot))
        for ok, copy in copies:
            @pl.when(both(ok, more))
            def _(copy=copy):
                copy.start()

    def wait_chunk_sends(slot, cond):
        copies = [(ok, remote(cs.at[slot, m], cr.at[slot, m], csend.at[slot, m], csend.at[slot, m], dev))
                  for m, (ok, dev) in enumerate(sides)]
        copies += corner_sends(0, slot) + corner_sends(n_chunks - 1, slot)
        for ok, copy in copies:
            @pl.when(both(ok, cond))
            def _(copy=copy):
                copy.wait_send()

    def wait_row_send(k, slot):
        ok, copy = row_send(k, slot)

        @pl.when(ok)
        def _():
            copy.wait_send()

    def wait_if(ok, dst, sem, src):
        @pl.when(ok)
        def _():
            remote(src, dst, csend.at[0, 0], sem, right_dev).wait_recv()

    sub48 = lax.broadcasted_iota(jnp.int32, (tile_w, ch), 0)
    sub16 = lax.broadcasted_iota(jnp.int32, (16, ch), 0)

    def row_of(colbuf, i):
        return cb[colbuf, pl.ds(i + 8, 1), :]

    def publish(slot, i, v, k):
        hb[slot, 1, i + 2] = v.astype(BF16)
        hb[slot, 0, i + 2] = pltpu.roll(v, 1, 0).astype(BF16)
        hb[slot, 2, i + 2] = pltpu.roll(v, tile_w - 1, 0).astype(BF16)
        j = i - starts[k]
        for side, m, x in edge_cells:
            cs[slot, side, k, j // PART, pl.ds(PART * m + j % PART, 1), :] = v[x:x + 1]
        cb[2, pl.ds(i + 8, 1), :] = v[0:1]
        cb[3, pl.ds(i + 8, 1), :] = v[tile_w - 1:tile_w]

    def wait_cols(slot, k, p):
        for m, (ok, _) in enumerate(sides):
            wait_if(ok, cr.at[slot, m, k, p], crecv.at[slot, m, k, p], cs.at[slot, 0, k, p])

    def place_cols(slot, k, p):
        i0, n = n_ranges[k]
        n = min(n - p * PART, PART)
        i0 = i0 + p * PART
        for side in range(2):
            for m in range(2):
                cb[4 * side + m, pl.ds(i0 + 8, n), :] = cr[slot, side, k, p, PART * m:PART * m + n, :]
        for i in range(i0, i0 + n):
            old = hb[slot, 0, i + 2, 0:16].astype(F32)
            hb[slot, 0, i + 2, 0:16] = jnp.where(sub16 == 0, row_of(1, i), old).astype(BF16)
            old = hb[slot, 2, i + 2, tile_w - 16:tile_w].astype(F32)
            hb[slot, 2, i + 2, tile_w - 16:tile_w] = jnp.where(sub16 == 15, row_of(4, i), old).astype(BF16)

    def wait_rows(slot, last):
        src, ok = (hl, has_last) if last else (hf, has_first)
        wait_if(ok, src.at[slot], vrecv.at[slot, last], h32.at[pl.ds(0, 2)])
        for m in range(2):
            q = 2 * last + m
            wait_if(corner_ok[q], kr.at[slot, q], krecv.at[slot, q], cs.at[slot, 0, 0, 0])

    def place_rows(slot, last):
        src = hl if last else hf
        for depth in range(2):
            i = tile_h + depth if last else -1 - depth
            m = 1 - depth if last else depth
            j = (CHUNKS[-1] - 1 - depth if last else depth) % PART
            for x in range(2):
                cb[x, pl.ds(i + 8, 1), :] = kr[slot, 2 * last, PART * x + j:PART * x + j + 1, :]
                cb[4 + x, pl.ds(i + 8, 1), :] = kr[slot, 2 * last + 1, PART * x + j:PART * x + j + 1, :]
            v = src[slot, m]
            cb[2, pl.ds(i + 8, 1), :] = v[0:1]
            cb[3, pl.ds(i + 8, 1), :] = v[tile_w - 1:tile_w]
            hb[slot, 1, i + 2] = v.astype(BF16)
            hb[slot, 0, i + 2] = jnp.where(sub48 == 0, row_of(1, i), pltpu.roll(v, 1, 0)).astype(BF16)
            hb[slot, 2, i + 2] = jnp.where(sub48 == tile_w - 1, row_of(4, i), pltpu.roll(v, tile_w - 1, 0)).astype(BF16)

    wide = tile_w + 2 * COL_HALO

    def build_x(t, k):
        i0, n = r_ranges[k]
        for j in range(n):
            parts = [pltpu.roll(fp[i0 + j + a + 1], lax.rem(cin * a - cin * t + cin * steps, cin * steps), 1) for a in range(3)]
            af[pl.ds(j * wide, wide)] = jnp.where(lane < cin, parts[0], jnp.where(lane < 2 * cin, parts[1], parts[2]))
        for j in range(n):
            base = j * wide + COL_HALO
            left = af[pl.ds(base - 1, tile_w)]
            mid = pltpu.roll(af[pl.ds(base, tile_w)], 64, 1)
            xp[i0 + j + 1, :, 0:LANES] = jnp.where(lane < 64, left, mid).astype(BF16)
            xp[i0 + j + 1, :, LANES:2 * LANES] = af[pl.ds(base + 1, tile_w)].astype(BF16)
        lo_half, hi_half = [], []
        for x in (-1, tile_w):
            three = [af[pl.ds(COL_HALO + x + c - 1, 8, wide)] for c in range(3)]
            lo_half.append(jnp.where(lane < 64, three[0], pltpu.roll(three[1], 64, 1)))
            hi_half.append(three[2])
        xe[k, :, 0:LANES] = jnp.concatenate(lo_half, axis=0).astype(BF16)
        xe[k, :, LANES:2 * LANES] = jnp.concatenate(hi_half, axis=0).astype(BF16)

    all_taps = ["x"] + [(a, c) for c in (1, 0, 2) for a in range(3)]

    def conv(src, i0, n, off, weights, gate, extra=None, e_lo=0, taps=all_taps, acc=None):
        lo, w_lo = gate * ch, (0 if gate == 2 else gate * ch)
        for tap in taps:
            if tap == "x":
                lhs = xp[pl.ds(i0 + 1, n)].reshape(n * tile_w, ch)
                more = None if extra is None else xe[extra]
                weight = wx[:, lo:lo + ch]
            else:
                a, c = tap
                lhs = src(c, pl.ds(i0 + a - 1 - off, n)).reshape(n * tile_w, ch)
                more = None if extra is None else jnp.concatenate(
                    [cb[3 * side + c, pl.ds(e_lo + a - 1 + 8, 8), :] for side in range(2)], axis=0).astype(BF16)
                weight = weights[a, c, :, w_lo:w_lo + ch]
            if more is not None:
                lhs = jnp.concatenate([lhs, more], axis=0)
            part = jnp.dot(lhs, weight, preferred_element_type=F32)
            acc = part if acc is None else acc + part
        return acc

    def biased(acc, gate):
        return acc + bv[gate * ch:(gate + 1) * ch].reshape(1, ch)

    for copy in frame_loads:
        copy.wait()
    pack_frames()
    f_descs = frame_copies()
    pl.semaphore_wait(barrier, count)
    for ok, copy, _, _ in f_descs:
        @pl.when(ok)
        def _(copy=copy):
            copy.start()
    for group in ((0, 1), range(2, n_chunks)):
        for k in group:
            loads[k].wait()
        for k in group:
            i0, n = n_ranges[k]
            for i in range(i0, i0 + n):
                v = hraw[phys(i)]
                h32[i] = v
                publish(0, i, v, k)
        for k in group:
            start_sends(k, 0, True)
    for ok, copy, _, _ in f_descs:
        @pl.when(ok)
        def _(copy=copy):
            copy.wait_send()
    for copy in weight_loads:
        copy.wait()
    for ok, copy, dst, sem in f_descs:
        @pl.when(ok)
        def _(dst=dst, sem=sem):
            remote(dst, dst, fsend.at[0], sem, right_dev).wait_recv()
    place_frames()
    build_x(0, 0)

    def halves(i0, n):
        return (i0, n - n // 2), (i0 + n - n // 2, n // 2)

    def meet(t, now, k):
        new = 1 - now
        if k == 0:
            start_sends(n_chunks - 1, now, both(t > 0, True))
            free_slot(t, now)
            wait_rows(now, 0)
            wait_row_send(0, now)
        else:
            start_sends(k - 1, new, t < steps - 1)
        fresh = [(k, p) for p in chunk_parts(k) if p or not k]
        if k + 1 < n_chunks:
            fresh.append((k + 1, 0))
        else:
            wait_rows(now, 1)
            wait_row_send(n_chunks - 1, now)
        for item in fresh:
            wait_cols(now, *item)
        for item in fresh:
            place_cols(now, *item)
        if k == 0:
            place_rows(now, 0)
        if k + 1 == n_chunks:
            place_rows(now, 1)

    def free_slot(t, now):
        new = 1 - now
        wait_chunk_sends(new, t >= 1)

    def ahead(now, k):
        out = []
        for h, (i0, n) in enumerate(halves(*n_ranges[k])):
            skip = 0 if k == 0 and h == 0 else 2 if k == n_chunks - 1 and h == 1 else None
            taps = [tap for tap in all_taps[:AHEAD] if tap == "x" or tap[0] != skip]
            acc = conv(lambda c, rows: hb[now, c, rows], i0, n, -2, wzr, 0, taps=taps)
            out.append((taps, acc))
        return out

    def stretch(t, now, k, begun, carry_on):
        new = 1 - now
        meet(t, now, k)
        r_lo, r_n = r_ranges[k]
        parts = halves(r_lo, r_n)
        accs = [conv(lambda c, rows: hb[now, c, rows], i0, n, -2, wzr, 1, extra=k if h == k % 2 else None, e_lo=r_lo) for h, (i0, n) in enumerate(parts)]
        gates = [sigmoid(biased(acc, 1)) for acc in accs]
        ends = gates[k % 2][parts[k % 2][1] * tile_w:]
        ends_l = ends[0:8] * cb[1, pl.ds(r_lo + 8, 8), :]
        ends_r = ends[8:16] * cb[4, pl.ds(r_lo + 8, 8), :]
        for (i0, n), gate in zip(parts, gates):
            for j in range(n):
                i = i0 + j
                e = i - r_lo
                old = hf[now, 0] if i == -1 else hl[now, 1] if i == tile_h else h32[i]
                v = gate[j * tile_w:(j + 1) * tile_w] * old
                rb[1, i + 1] = v.astype(BF16)
                rb[0, i + 1] = jnp.where(sub48 == 0, ends_l[e:e + 1], pltpu.roll(v, 1, 0)).astype(BF16)
                rb[2, i + 1] = jnp.where(sub48 == tile_w - 1, ends_r[e:e + 1], pltpu.roll(v, tile_w - 1, 0)).astype(BF16)
        parts = halves(*n_ranges[k])
        for h, (i0, n) in enumerate(parts):
            done, acc = begun[h] if begun is not None else ([], None)
            acc = conv(lambda c, rows: hb[now, c, rows], i0, n, -2, wzr, 0, taps=[tap for tap in all_taps if tap not in done], acc=acc)
            zb[pl.ds((i0 - n_ranges[k][0]) * tile_w, n * tile_w)] = sigmoid(biased(acc, 0))
        if k + 1 < n_chunks:
            build_x(t, k + 1)
        else:
            build_x(jnp.minimum(t + 1, steps - 1), 0)
        accs = [conv(lambda c, rows: rb[c, rows], i0, n, -1, wn, 2) for i0, n in parts]
        begun = None
        if carry_on and k + 1 < n_chunks:
            begun = ahead(now, k + 1)
        for (i0, n), acc in zip(parts, accs):
            cand = jnp.tanh(biased(acc, 2))
            for j in range(n):
                i = i0 + j
                mix = cand[j * tile_w:(j + 1) * tile_w]
                v = mix + zb[pl.ds((i - n_ranges[k][0]) * tile_w, tile_w)] * (h32[i] - mix)
                h32[i] = v
                h_seq[t, 0, phys(i)] = v.astype(BF16)
                publish(new, i, v, k)
        if carry_on and k + 1 == n_chunks:
            begun = ahead(new, 0)
        return begun

    def body(p, carry):
        begun = None
        for s in range(UNROLL):
            for k in range(n_chunks):
                last = s == UNROLL - 1 and k == n_chunks - 1
                begun = stretch(UNROLL * p + s, s % 2, k, begun, not last)
        return carry

    lax.fori_loop(0, steps // UNROLL, body, 0)
    wait_chunk_sends((steps - 1) % 2, True)
    for i in range(tile_h):
        h_last[0, phys(i)] = h32[i]


def solution(mesh):
    n_rows, n_cols = mesh.shape["rows"], mesh.shape["cols"]
    frame_spec = P(None, "batch", "rows", "cols", None)
    state_spec = P("batch", "rows", "cols", None)

    def local_fn(frames, h_init, w_x, w_hzr, w_hn, gate_bias):
        steps, _, tile_h, tile_w, cin = frames.shape
        ch = h_init.shape[-1]
        dims = (steps, tile_h, tile_w, cin, ch)
        vm = pltpu.VMEM
        dma = pltpu.SemaphoreType.DMA
        kk = len(CHUNKS)
        wide = tile_w + 2 * COL_HALO
        pair = (2, 2)
        scratch = [
            vm((3, 3, ch, 2 * ch), BF16), vm((3, 3, ch, ch), BF16), vm((256, 3 * ch), BF16), vm((3 * ch,), F32),
            vm((steps, tile_h, cin, tile_w), BF16), vm((tile_h + 4, wide, LANES), F32),
            vm(pair + (tile_h, LANES), F32), vm(pair + (tile_h, LANES), F32), vm((4, 2, 8, LANES), F32),
            vm((2, 3, tile_h + 4, tile_w, ch), BF16), vm((3, tile_h + 2, tile_w, ch), BF16),
            vm((tile_h + 2, tile_w, ch), BF16), vm((kk, 16, ch), BF16), vm((8 * wide, LANES), F32),
            vm((tile_h, tile_w, ch), F32), vm((tile_h, tile_w, ch), F32), vm((max(CHUNKS) * tile_w, ch), F32),
            vm(pair + (tile_w, ch), F32), vm(pair + (tile_w, ch), F32),
            vm(pair + (kk, 3, 2 * PART, ch), F32), vm(pair + (kk, 3, 2 * PART, ch), F32), vm((2, 4, 2 * PART, ch), F32), vm((6, 48, ch), F32),
            dma((3, tile_h)), dma((10,)), dma((10,)), dma(pair), dma(pair + (kk, 3)), dma((2, 4)), dma((2, 4)),
            dma((2,)), dma(pair),
        ]

        def body(*refs):
            kernel_body(n_cols, n_rows, dims, *refs)

        results = pl.pallas_call(
            body,
            out_shape=(vm((steps, 1, tile_h, tile_w, ch), BF16), vm((1, tile_h, tile_w, ch), F32)),
            in_specs=[pl.BlockSpec(memory_space=pltpu.HBM)] * 6,
            out_specs=(pl.BlockSpec(memory_space=vm),) * 2,
            scratch_shapes=scratch,
            compiler_params=pltpu.CompilerParams(collective_id=0, has_side_effects=True, vmem_limit_bytes=VMEM_LIMIT),
            name="convgru",
        )(*[pltpu.with_memory_space_constraint(v, pltpu.HBM) for v in (jnp.swapaxes(frames, 3, 4), h_init, w_x, w_hzr, w_hn, gate_bias)])

        def drain(seq_in, last_in, seq_out, last_out, sems):
            copies = [pltpu.make_async_copy(src, dst, sems.at[m]) for m, (src, dst) in enumerate(((seq_in, seq_out), (last_in, last_out)))]
            for copy in copies:
                copy.start()
            for copy in copies:
                copy.wait()

        return pl.pallas_call(
            drain,
            out_shape=[jax.ShapeDtypeStruct(v.shape, v.dtype) for v in results],
            in_specs=[pl.BlockSpec(memory_space=vm)] * 2,
            out_specs=[pl.BlockSpec(memory_space=pltpu.HBM)] * 2,
            scratch_shapes=[dma((2,))],
            compiler_params=pltpu.CompilerParams(vmem_limit_bytes=VMEM_LIMIT // 8),
            name="drain",
        )(*[pltpu.with_memory_space_constraint(v, vm) for v in results])

    return jax.shard_map(local_fn, mesh=mesh, in_specs=(frame_spec, state_spec, P(), P(), P(), P()), out_specs=(frame_spec, state_spec), check_vma=False)
```
